32 devices in a mesh: span: 8 (over y, x, core), head: 4 (over z).
Axes of the slice: x: 2, y: 2, z: 4, core: 2. Of those that a mesh axis runs over, the one named last changes fastest.
Arguments:
- decoder_states: bfloat16 [16384, 1024], P('span'), may hold values from -21 to 21
- encodings: bfloat16 [512, 128, 1024], P('span', 'head'), may hold values from -21 to 21
- neighbor_table: int32 [256, 2, 2], P('span'), may hold values from 0 to 63, as said below
- query_weight: bfloat16 [1024, 1024], P(None, 'head'), may hold values from -0.1875 to 0.1875
- key_weight: bfloat16 [1024, 1024], P(None, 'head'), may hold values from -0.1875 to 0.1875
- value_weight: bfloat16 [1024, 1024], P(None, 'head'), may hold values from -0.1875 to 0.1875
- out_weight: bfloat16 [1024, 1024], P('head'), may hold values from -0.1875 to 0.1875
Outputs:
- attended: bfloat16 [16384, 1024], P('span', 'head')
The draws below stay inside these ranges and needn't reach their ends.
Inputs may be any that keep to these rules, and one draw needn't show every extreme that they name: neighbor_table[c, k, 0] is the database shard and neighbor_table[c, k, 1] the slot in that shard of neighbor k of span c; in each aligned block of 32 spans (the spans of one device along `span`) every shard is named by exactly one neighbor, and every slot of every shard is named exactly once in the whole table.
All inputs are finite; a program needn't handle non-finite values.
Results may differ from the reference program's by a relative error of at most 0.012.
The reference program's roundings to bfloat16 on the way (of `keys`, `values`, `queries`, `weights` and `context`) count: a program that leaves them out, or rounds other values in their place, can miss the bound.
Values may be sent and summed in bfloat16 or wider, within the bound.
A program may use at most 128 MiB of HBM per device.

```python
import jax
import jax.numpy as jnp
from jax import lax

D = 1024
HEADS = 16
HEAD_DIM = 64
SPAN_LEN = 64
NEIGH = 2
NTOK = 128
SEQ_LEN = 2048
SPANS_SEQ = 32
TOKENS = 16384
SPANS = 256
SHARDS = 8
SLOTS = 64
PER_SOURCE = 8


def draw_decoder_states(key, part):
    subkeys = jax.random.split(jax.random.fold_in(key, 3), 1)
    values = jnp.clip(jax.random.normal(subkeys[0], (TOKENS, D), jnp.float32), -6.0, 6.0)
    return values.astype(jnp.bfloat16)


def draw_encodings(key, part):
    subkeys = jax.random.split(jax.random.fold_in(key, 5), 1)
    shape_all = (SHARDS * SLOTS, NTOK, D)
    values = jnp.clip(jax.random.normal(subkeys[0], shape_all, jnp.float32), -6.0, 6.0)
    return values.astype(jnp.bfloat16)


def draw_neighbor_table(key, part):
    dest_keys = jax.random.split(jax.random.fold_in(key, 11), SHARDS)
    orders = jax.vmap(lambda subkey: jax.random.permutation(subkey, SLOTS))(dest_keys).astype(jnp.int32)
    shard_of = orders // PER_SOURCE
    sub_index = orders % PER_SOURCE
    source_keys = jax.random.split(jax.random.fold_in(key, 12), SHARDS)
    slot_orders = jax.vmap(lambda subkey: jax.random.permutation(subkey, SLOTS))(source_keys).astype(jnp.int32)
    destination = jnp.arange(SHARDS, dtype=jnp.int32)[:, None]
    slot_of = slot_orders[shard_of, destination * PER_SOURCE + sub_index]
    return jnp.stack([shard_of, slot_of], axis=-1).reshape(SPANS, NEIGH, 2).astype(jnp.int32)


def steps_of(rng, dims, pieces, smallest, largest):
    def one(position, parts):
        draws = jax.random.uniform(jax.random.fold_in(jax.random.fold_in(rng, 6), position), (parts,), jnp.float32, smallest / len(pieces), largest / len(pieces))
        return jnp.repeat(jnp.exp(draws), dims[position] // parts).reshape((-1,) + (1,) * (len(dims) - position - 1))

    level = one(*pieces[0])
    for cut in pieces[1:]:
        level = level * one(*cut)
    return level


def normal_values(key, dims, spread, bound, pieces=(), kind=jnp.bfloat16):
    drawn = jax.random.normal(key, dims, jnp.float32) * spread
    if len(pieces) > 0:
        drawn = steps_of(key, dims, pieces, -0.22, 0.18) * drawn
    return jnp.clip(drawn, min=-bound, max=bound).astype(kind)


def setup_inputs(seed: int = 0) -> dict:
    keys = jax.random.split(jax.random.key(seed), 8)
    decoder_states = draw_decoder_states(jax.random.fold_in(keys[7], 71), 0)
    encodings = draw_encodings(jax.random.fold_in(keys[7], 71), 0)
    neighbor_table = draw_neighbor_table(jax.random.fold_in(keys[7], 71), 0)
    query_weight = normal_values(keys[3], (D, HEADS * HEAD_DIM), D ** -0.5, 0.1875, ((1, 4),))
    key_weight = normal_values(keys[4], (D, HEADS * HEAD_DIM), D ** -0.5, 0.1875, ((1, 4),))
    value_weight = normal_values(keys[5], (D, HEADS * HEAD_DIM), D ** -0.5, 0.1875, ((1, 4),))
    out_weight = normal_values(keys[6], (HEADS * HEAD_DIM, D), (HEADS * HEAD_DIM) ** -0.5, 0.1875, ((0, 4),))
    return dict(decoder_states=decoder_states, encodings=encodings, neighbor_table=neighbor_table, query_weight=query_weight, key_weight=key_weight, value_weight=value_weight, out_weight=out_weight)


def reference(decoder_states, encodings, neighbor_table, query_weight, key_weight, value_weight, out_weight):
    group_rows = (neighbor_table[:, :, 0] * SLOTS + neighbor_table[:, :, 1]).astype(jnp.int32)
    inv_root = HEAD_DIM ** -0.5
    offset = SPAN_LEN - 1
    inner_width = HEADS * HEAD_DIM

    def one_sequence(sequence):
        states = lax.dynamic_slice_in_dim(decoder_states, sequence * SEQ_LEN, SEQ_LEN, 0)
        chosen = lax.dynamic_slice_in_dim(group_rows, sequence * SPANS_SEQ, SPANS_SEQ, 0).reshape(-1)
        flattened = encodings[chosen].reshape(-1, D)
        key_rows = jnp.dot(flattened, key_weight, preferred_element_type=jnp.float32).astype(jnp.bfloat16)
        key_rows = key_rows.reshape(SPANS_SEQ, NEIGH * NTOK, HEADS, HEAD_DIM)
        value_rows = jnp.dot(flattened, value_weight, preferred_element_type=jnp.float32).astype(jnp.bfloat16)
        value_rows = value_rows.reshape(SPANS_SEQ, NEIGH * NTOK, HEADS, HEAD_DIM)
        queries = jnp.dot(states, query_weight, preferred_element_type=jnp.float32).astype(jnp.bfloat16)
        shifted = jnp.concatenate([queries[offset:], jnp.zeros((offset, inner_width), jnp.bfloat16)], axis=0)
        shifted = shifted.reshape(SPANS_SEQ, SPAN_LEN, HEADS, HEAD_DIM)
        scores = jnp.einsum("cqhd,ckhd->chqk", shifted.astype(jnp.float32), key_rows.astype(jnp.float32)) * inv_root
        weights = jax.nn.softmax(scores, axis=-1).astype(jnp.bfloat16)
        context = jnp.einsum("chqk,ckhd->cqhd", weights.astype(jnp.float32), value_rows.astype(jnp.float32))
        context = context.astype(jnp.bfloat16).reshape(SEQ_LEN, inner_width)
        context = jnp.concatenate([jnp.zeros((offset, inner_width), jnp.bfloat16), context[:SEQ_LEN - offset]], axis=0)
        return jnp.dot(context, out_weight, preferred_element_type=jnp.float32).astype(jnp.bfloat16)

    sequences = TOKENS // SEQ_LEN
    outputs = lax.map(one_sequence, jnp.arange(sequences, dtype=jnp.int32))
    return outputs.reshape(TOKENS, D)
```

```python
import functools

import jax
import jax.numpy as jnp
from jax import lax
from jax.experimental import pallas as pl
from jax.experimental.pallas import tpu as pltpu
from jax.sharding import PartitionSpec as P

HEAD_DIM = 64
SPAN_LEN = 64
SEQ_LEN = 2048
VMEM = 63 * 1024 * 1024
CHUNK_SPANS = 4
LINK = pl.DeviceIdType.MESH


def flip(index, bits, size):
    out = 0
    weight = 1
    while weight < size:
        out = out + weight * ((index // weight + bits // weight) % 2)
        weight *= 2
    return out


def kernel(
    span_size,
    head_size,
    position_ref,
    request_ref,
    states_hbm,
    encodings_hbm,
    query_hbm,
    key_hbm,
    value_hbm,
    out_hbm,
    o_ref,
    enc,
    sent,
    arrived,
    weights,
    outs,
    states,
    queries,
    kv,
    own,
    right,
    left,
    lse,
    top,
    ctx,
    score,
    expo,
    final,
    asked,
    asked_s,
    local_sem,
    ask_send,
    ask_recv,
    enc_send,
    enc_recv,
    line_send,
    line_recv,
    pair_send,
    pair_recv,
    lse_send,
    lse_recv,
    right_send,
    right_recv,
    left_send,
    left_recv,
):
    me = lax.axis_index("span")
    plane = lax.axis_index("head")
    core = me % 2
    partner = me + 1 - 2 * core
    slots, tokens, model = encodings_hbm.shape
    per_peer = kv.shape[1] // span_size
    group = query_hbm.shape[1]
    last = head_size - 1

    own_copies = [
        pltpu.make_async_copy(key_hbm, weights.at[plane, :, 0:group], local_sem.at[0]),
        pltpu.make_async_copy(value_hbm, weights.at[plane, :, group : 2 * group], local_sem.at[1]),
        pltpu.make_async_copy(query_hbm, weights.at[plane, :, 2 * group : 3 * group], local_sem.at[2]),
        pltpu.make_async_copy(encodings_hbm, enc, local_sem.at[3]),
        pltpu.make_async_copy(states_hbm, states, local_sem.at[4]),
        pltpu.make_async_copy(out_hbm, outs.at[plane], local_sem.at[5]),
    ]
    for copy in own_copies:
        copy.start()
    asked[me] = request_ref[me]

    barrier = pltpu.get_barrier_semaphore()
    for k in range(1, span_size):
        pl.semaphore_signal(
            barrier, inc=1, device_id=(flip(me, k, span_size), plane), device_id_type=LINK
        )
    for k in range(1, head_size):
        pl.semaphore_signal(
            barrier, inc=1, device_id=(me, (plane + k) % head_size), device_id_type=LINK
        )
    pl.semaphore_wait(barrier, span_size + head_size - 2)

    def ask(k):
        peer = flip(me, k, span_size)
        return pltpu.make_async_remote_copy(
            src_ref=request_ref.at[peer],
            dst_ref=asked.at[me],
            send_sem=ask_send.at[k],
            recv_sem=ask_recv.at[k],
            device_id=(peer, plane),
            device_id_type=LINK,
        )

    def landed(k):
        peer = flip(me, k, span_size)
        return pltpu.make_async_remote_copy(
            src_ref=request_ref.at[peer],
            dst_ref=asked.at[peer],
            send_sem=ask_send.at[k],
            recv_sem=ask_recv.at[k],
            device_id=(peer, plane),
            device_id_type=LINK,
        )

    for k in range(1, span_size):
        ask(k).start()

    halves = ((weights, weights.shape[1] // 2, 0), (outs, outs.shape[1] // 2, 1))

    def line_copy(which, shard, to, direction):
        buf, half, slot = halves[which]
        rows = pl.ds(pl.multiple_of(core * half, half), half)
        return pltpu.make_async_remote_copy(
            src_ref=buf.at[shard, rows],
            dst_ref=buf.at[shard, rows],
            send_sem=line_send.at[slot, shard, direction],
            recv_sem=line_recv.at[slot, shard],
            device_id=(me, to),
            device_id_type=LINK,
        )

    def pair_copy(which, shard):
        buf, half, slot = halves[which]
        rows = pl.ds(pl.multiple_of(core * half, half), half)
        return pltpu.make_async_remote_copy(
            src_ref=buf.at[shard, rows],
            dst_ref=buf.at[shard, rows],
            send_sem=pair_send.at[slot, shard],
            recv_sem=pair_recv.at[slot, shard],
            device_id=(partner, plane),
            device_id_type=LINK,
        )

    def pair_landed(which, shard):
        buf, half, slot = halves[which]
        rows = pl.ds(pl.multiple_of((1 - core) * half, half), half)
        return pltpu.make_async_remote_copy(
            src_ref=buf.at[shard, rows],
            dst_ref=buf.at[shard, rows],
            send_sem=pair_send.at[slot, shard],
            recv_sem=pair_recv.at[slot, shard],
            device_id=(partner, plane),
            device_id_type=LINK,
        )

    def send_own(which):
        @pl.when(plane < last)
        def _():
            line_copy(which, plane, plane + 1, 0).start()

        @pl.when(plane > 0)
        def _():
            line_copy(which, plane, plane - 1, 1).start()

    def pass_on(which, k):
        @pl.when(plane - k >= 0)
        def _():
            shard = plane - k
            line_copy(which, shard, plane, 0).wait_recv()

            @pl.when(plane < last)
            def _():
                line_copy(which, shard, plane + 1, 0).start()

            pair_copy(which, shard).start()

        @pl.when(plane + k <= last)
        def _():
            shard = plane + k
            line_copy(which, shard, plane, 1).wait_recv()

            @pl.when(plane > 0)
            def _():
                line_copy(which, shard, plane - 1, 1).start()

            pair_copy(which, shard).start()

    for copy in own_copies[:3]:
        copy.wait()
    send_own(0)

    for k in range(1, span_size):
        landed(k).wait_recv()
    to_scalar = pltpu.make_async_copy(asked, asked_s, local_sem.at[6])
    to_scalar.start()
    own_copies[3].wait()
    to_scalar.wait()

    def enc_copy(k):
        peer = flip(me, k, span_size)
        return pltpu.make_async_remote_copy(
            src_ref=sent.at[peer],
            dst_ref=arrived.at[me],
            send_sem=enc_send.at[k],
            recv_sem=enc_recv.at[k],
            device_id=(peer, plane),
            device_id_type=LINK,
        )

    def enc_landed(k):
        peer = flip(me, k, span_size)
        return pltpu.make_async_remote_copy(
            src_ref=sent.at[peer],
            dst_ref=arrived.at[peer],
            send_sem=enc_send.at[k],
            recv_sem=enc_recv.at[k],
            device_id=(peer, plane),
            device_id_type=LINK,
        )

    def pick(buf, peer):
        for j in range(per_peer):
            buf[peer, j] = enc[asked_s[peer, 0, j]]

    def pick_and_send(k, carry):
        pick(sent, flip(me, k, span_size))

        @pl.when(k > 1)
        def _():
            enc_copy(k - 1).start()

        return carry

    lax.fori_loop(1, span_size, pick_and_send, 0)
    pick(arrived, me)
    enc_copy(span_size - 1).start()

    own_copies[4].wait()
    blocks, block_len, _ = states.shape
    blocks_seq = SEQ_LEN // block_len
    row = lax.broadcasted_iota(jnp.int32, (block_len, model), 0)

    def move_up(b, carry):
        inside = (b + 1) % blocks_seq != 0
        following = states[(b + 1) % blocks].astype(jnp.float32)
        following = jnp.where(inside, following, 0.0)
        tail = states[b].astype(jnp.float32)[block_len - 1 :]
        moved = jnp.where(row == 0, tail, pltpu.roll(following, 1, 0))
        states[b] = moved.astype(states.dtype)
        return carry

    lax.fori_loop(0, blocks, move_up, 0)

    def project_queries(shard):
        step = min(4, blocks)

        def one(b, carry):
            x = states[pl.ds(b * step, step)].reshape(step * block_len, model)
            y = jnp.dot(
                x, weights[shard, :, 2 * group : 3 * group], preferred_element_type=jnp.float32
            )
            queries[shard, pl.ds(b * step, step)] = y.astype(queries.dtype).reshape(
                step, block_len, group
            )
            return carry

        lax.fori_loop(0, blocks // step, one, 0)

    def project_keys(shard, first, end):
        def one(k, carry):
            peer = flip(me, k, span_size)
            x = arrived[peer].reshape(per_peer * tokens, model)
            y = jnp.dot(x, weights[shard, :, 0 : 2 * group], preferred_element_type=jnp.float32)
            kv[shard, pl.ds(peer * per_peer, per_peer)] = y.astype(kv.dtype).reshape(
                per_peer, tokens, 2 * group
            )
            return carry

        lax.fori_loop(first, end, one, 0)

    def shards_at(k, work):
        if k == 0:
            work(plane)
            return

        @pl.when(plane - k >= 0)
        def _():
            work(plane - k)

        @pl.when(plane + k <= last)
        def _():
            work(plane + k)

    near, mid = span_size // 4, span_size - span_size // 4
    bounds = (0, near, mid, span_size)

    def keys_of(k, a, b):
        shards_at(k, lambda shard: project_keys(shard, bounds[a], bounds[b]))

    def wait_enc(a):
        for k in range(max(bounds[a], 1), bounds[a + 1]):
            enc_landed(k).wait_recv()

    def wait_pair(which, k):
        shards_at(k, lambda shard: pair_landed(which, shard).wait_recv())

    project_queries(plane)
    wait_enc(0)
    keys_of(0, 0, 1)
    for k in range(1, last):
        pass_on(0, k)
        if k == last - 1:
            own_copies[5].wait()
            send_own(1)
        wait_pair(0, k)
        shards_at(k, project_queries)
        keys_of(k, 0, 1)
        if k == 1:
            wait_enc(1)
            keys_of(0, 1, 2)
            keys_of(1, 1, 2)
        else:
            keys_of(k, 1, 2)
    wait_enc(2)
    for k in range(last):
        keys_of(k, 2, 3)
    pass_on(0, last)
    wait_pair(0, last)
    shards_at(last, project_queries)
    keys_of(last, 0, 3)
    for k in range(1, head_size):
        pass_on(1, k)
    for k in range(1, head_size):
        wait_pair(1, k)

    chunks = right.shape[0]
    chunk_spans = CHUNK_SPANS
    heads = head_size * group // HEAD_DIM
    neighbors = position_ref.shape[0] // blocks
    keys = neighbors * tokens
    packed = group // HEAD_DIM
    wide = packed * keys
    diagonal = (
        lax.broadcasted_iota(jnp.int32, (wide, group), 0) // keys
        == lax.broadcasted_iota(jnp.int32, (wide, group), 1) // HEAD_DIM
    )
    pair = 128 // keys
    lane = lax.broadcasted_iota(jnp.int32, (SPAN_LEN, 128), 1)
    lane_head = lane // keys
    collect = (
        lax.broadcasted_iota(jnp.int32, (heads * keys, 128), 0) // keys
        == lax.broadcasted_iota(jnp.int32, (heads * keys, 128), 1)
    ).astype(jnp.bfloat16)

    def attend(chunk):
        def widened(c, g, base):
            part = jnp.concatenate(
                [
                    kv[g, position_ref[(chunk * chunk_spans + c) * neighbors + n]][
                        :, base : base + group
                    ]
                    for n in range(neighbors)
                ],
                axis=0,
            )
            return jnp.where(diagonal, jnp.concatenate([part] * packed, axis=0), 0)

        for c in range(chunk_spans):
            rows = slice(c * SPAN_LEN, (c + 1) * SPAN_LEN)
            for g in range(head_size):
                score[rows, g * wide : (g + 1) * wide] = lax.dot_general(
                    queries[g, chunk * chunk_spans + c],
                    widened(c, g, 0),
                    (((1,), (1,)), ((), ())),
                    preferred_element_type=jnp.float32,
                ) * (HEAD_DIM ** (-0.5))
        tops = []
        for c in range(chunk_spans):
            rows = slice(c * SPAN_LEN, (c + 1) * SPAN_LEN)
            top_all = jnp.zeros((SPAN_LEN, 128), jnp.float32)
            for t in range(heads // pair):
                s = score[rows, t * 128 : (t + 1) * 128]
                peak = None
                for n in range(pair):
                    m = jnp.max(jnp.where(lane_head == n, s, -jnp.inf), axis=1, keepdims=True)
                    peak = m if peak is None else jnp.where(lane_head == n, m, peak)
                    top_all = jnp.where(lane == t * pair + n, m, top_all)
                expo[rows, t * 128 : (t + 1) * 128] = jnp.exp(s - peak).astype(jnp.bfloat16)
            tops.append(top_all)
        top_all = jnp.concatenate(tops, axis=0)
        total = jnp.dot(expo[...], collect, preferred_element_type=jnp.float32)
        top_rows = top_all.T[:heads]
        top[chunk % 2] = top_rows
        lse[plane, chunk] = top_rows + jnp.log(total.T[:heads])
        for c in range(chunk_spans):
            rows = slice(c * SPAN_LEN, (c + 1) * SPAN_LEN)
            for g in range(head_size):
                ctx[chunk % 2, rows, g * group : (g + 1) * group] = jnp.dot(
                    expo[rows, g * wide : (g + 1) * wide],
                    widened(c, g, group),
                    preferred_element_type=jnp.float32,
                ).astype(ctx.dtype)

    def lse_copy(chunk, k):
        return pltpu.make_async_remote_copy(
            src_ref=lse.at[plane, chunk],
            dst_ref=lse.at[plane, chunk],
            send_sem=lse_send.at[chunk, k],
            recv_sem=lse_recv.at[chunk, k],
            device_id=(me, (plane + k) % head_size),
            device_id_type=LINK,
        )

    def lse_landed(chunk, k):
        origin = (plane + head_size - k) % head_size
        return pltpu.make_async_remote_copy(
            src_ref=lse.at[origin, chunk],
            dst_ref=lse.at[origin, chunk],
            send_sem=lse_send.at[chunk, k],
            recv_sem=lse_recv.at[chunk, k],
            device_id=(me, (plane + k) % head_size),
            device_id_type=LINK,
        )

    def project(chunk):
        every = lse[:, chunk]
        highest = jnp.max(every, axis=0)
        total = jnp.sum(jnp.exp(every - highest[None]), axis=0)
        scale = jnp.exp(top[chunk % 2] - highest) / total
        high = scale.astype(jnp.bfloat16)
        low = (scale - high.astype(jnp.float32)).astype(jnp.bfloat16)
        spread = (
            lax.broadcasted_iota(jnp.int32, (2 * heads, model), 0) % heads
            == lax.broadcasted_iota(jnp.int32, (2 * heads, model), 1) // HEAD_DIM
        ).astype(jnp.bfloat16)
        factor = lax.dot_general(
            jnp.concatenate([high, low], axis=0),
            spread,
            (((0,), (0,)), ((), ())),
            preferred_element_type=jnp.float32,
        )
        scaled = (ctx[chunk % 2].astype(jnp.float32) * factor).astype(jnp.bfloat16)
        w = outs[...].reshape(head_size * group, model)
        y = jnp.dot(scaled, w, preferred_element_type=jnp.float32)
        for q in range(head_size):
            own[chunk % head_size, q] = y[:, q * group : (q + 1) * group]

    def right_copy(chunk, q, to):
        return pltpu.make_async_remote_copy(
            src_ref=right.at[chunk, q],
            dst_ref=right.at[chunk, q],
            send_sem=right_send.at[chunk, q],
            recv_sem=right_recv.at[chunk, q],
            device_id=(me, to),
            device_id_type=LINK,
        )

    def left_copy(chunk, q, to):
        return pltpu.make_async_remote_copy(
            src_ref=left.at[chunk, q],
            dst_ref=left.at[chunk, q],
            send_sem=left_send.at[chunk, q],
            recv_sem=left_recv.at[chunk, q],
            device_id=(me, to),
            device_id_type=LINK,
        )

    def step(it, carry):
        @pl.when(it < chunks)
        def _():
            attend(it)
            for k in range(1, head_size):
                lse_copy(it, k).start()

        @pl.when((it >= 1) & (it <= chunks))
        def _():
            for k in range(1, head_size):
                lse_landed(it - 1, k).wait_recv()
            project(it - 1)

        to_right = it - 1 - plane
        right_on = (to_right >= 0) & (to_right < chunks)
        to_left = it - 1 - (last - plane)
        left_on = (to_left >= 0) & (to_left < chunks)
        for q in range(head_size):

            @pl.when(right_on & (q > plane) & (plane == 0))
            def _():
                right[to_right, q] = own[to_right % head_size, q].astype(right.dtype)

            @pl.when(right_on & (q > plane) & (plane > 0))
            def _():
                right_copy(to_right, q, plane).wait_recv()
                right[to_right, q] = (
                    own[to_right % head_size, q] + right[to_right, q].astype(jnp.float32)
                ).astype(right.dtype)

            @pl.when(left_on & (q < plane) & (plane == last))
            def _():
                left[to_left, q] = own[to_left % head_size, q].astype(left.dtype)

            @pl.when(left_on & (q < plane) & (plane < last))
            def _():
                left_copy(to_left, q, plane).wait_recv()
                left[to_left, q] = (
                    own[to_left % head_size, q] + left[to_left, q].astype(jnp.float32)
                ).astype(left.dtype)

        for q in range(head_size):

            @pl.when(right_on & (q > plane))
            def _():
                right_copy(to_right, q, plane + 1).start()

            @pl.when(left_on & (q < plane))
            def _():
                left_copy(to_left, q, plane - 1).start()

        done = it - 1 - jnp.maximum(plane, last - plane)

        @pl.when((done >= 0) & (done < chunks))
        def _():
            @pl.when(plane == 0)
            def _():
                left_copy(done, plane, plane).wait_recv()
                put(done, own[done % head_size, plane] + left[done, plane].astype(jnp.float32))

            @pl.when(plane == last)
            def _():
                right_copy(done, plane, plane).wait_recv()
                put(done, own[done % head_size, plane] + right[done, plane].astype(jnp.float32))

            @pl.when((plane > 0) & (plane < last))
            def _():
                left_copy(done, plane, plane).wait_recv()
                right_copy(done, plane, plane).wait_recv()
                put(
                    done,
                    own[done % head_size, plane]
                    + left[done, plane].astype(jnp.float32)
                    + right[done, plane].astype(jnp.float32),
                )

        return carry

    def put(chunk, value):
        final[pl.ds(chunk * chunk_spans, chunk_spans)] = value.reshape(
            chunk_spans, SPAN_LEN, group
        )

    lax.fori_loop(0, chunks + head_size, step, 0)

    out_row = lax.broadcasted_iota(jnp.int32, (SPAN_LEN, group), 0)

    def move_down(b, carry):
        before = jnp.where(b % blocks_seq != 0, final[(b + blocks - 1) % blocks], 0.0)
        moved = jnp.where(
            out_row == SPAN_LEN - 1, final[b][0:1], pltpu.roll(before, SPAN_LEN - 1, 0)
        )
        o_ref[b] = moved.astype(o_ref.dtype)
        return carry

    lax.fori_loop(0, blocks, move_down, 0)

    for k in range(1, span_size):
        ask(k).wait_send()
        enc_copy(k).wait_send()
    for which in range(2):

        @pl.when(plane < last)
        def _():
            line_copy(which, plane, plane + 1, 0).wait_send()

        @pl.when(plane > 0)
        def _():
            line_copy(which, plane, plane - 1, 1).wait_send()

        for k in range(1, head_size):

            @pl.when(plane - k >= 0)
            def _():
                @pl.when(plane < last)
                def _():
                    line_copy(which, plane - k, plane + 1, 0).wait_send()

                pair_copy(which, plane - k).wait_send()

            @pl.when(plane + k <= last)
            def _():
                @pl.when(plane > 0)
                def _():
                    line_copy(which, plane + k, plane - 1, 1).wait_send()

                pair_copy(which, plane + k).wait_send()

    def drain(chunk, carry):
        for k in range(1, head_size):
            lse_copy(chunk, k).wait_send()
        for q in range(head_size):

            @pl.when(q > plane)
            def _():
                right_copy(chunk, q, plane + 1).wait_send()

            @pl.when(q < plane)
            def _():
                left_copy(chunk, q, plane - 1).wait_send()

        return carry

    lax.fori_loop(0, chunks, drain, 0)


def fused(
    position, request, states, encodings, query_weight, key_weight, value_weight, out_weight
):
    span_size = lax.axis_size("span")
    head_size = lax.axis_size("head")
    slots, tokens, model = encodings.shape
    rows = states.shape[0]
    group = query_weight.shape[1]
    entries = position.shape[0]
    per_peer = entries // span_size
    blocks = rows // SPAN_LEN
    chunks = blocks // CHUNK_SPANS
    chunk_rows = CHUNK_SPANS * SPAN_LEN
    heads = head_size * group // HEAD_DIM
    score_cols = heads * (entries // blocks) * tokens
    bf16, f32 = jnp.bfloat16, jnp.float32
    dma = pltpu.SemaphoreType.DMA
    vmem = pl.BlockSpec(memory_space=pltpu.VMEM)
    hbm = pl.BlockSpec(memory_space=pl.ANY)
    return pl.pallas_call(
        functools.partial(kernel, span_size, head_size),
        out_shape=jax.ShapeDtypeStruct((blocks, SPAN_LEN, group), bf16),
        in_specs=[pl.BlockSpec(memory_space=pltpu.SMEM), vmem] + [hbm] * 6,
        out_specs=vmem,
        scratch_shapes=[
            pltpu.VMEM((slots, tokens, model), bf16),
            pltpu.VMEM((span_size, per_peer, tokens, model), bf16),
            pltpu.VMEM((span_size, per_peer, tokens, model), bf16),
            pltpu.VMEM((head_size, model, 3 * group), bf16),
            pltpu.VMEM((head_size, group, model), bf16),
            pltpu.VMEM((blocks, SPAN_LEN, model), bf16),
            pltpu.VMEM((head_size, blocks, SPAN_LEN, group), bf16),
            pltpu.VMEM((head_size, entries, tokens, 2 * group), bf16),
            pltpu.VMEM((head_size, head_size, chunk_rows, group), f32),
            pltpu.VMEM((chunks, head_size, chunk_rows, group), bf16),
            pltpu.VMEM((chunks, head_size, chunk_rows, group), bf16),
            pltpu.VMEM((head_size, chunks, heads, chunk_rows), f32),
            pltpu.VMEM((2, heads, chunk_rows), f32),
            pltpu.VMEM((2, chunk_rows, model), bf16),
            pltpu.VMEM((chunk_rows, score_cols), f32),
            pltpu.VMEM((chunk_rows, score_cols), bf16),
            pltpu.VMEM((blocks, SPAN_LEN, group), f32),
            pltpu.VMEM(request.shape, jnp.int32),
            pltpu.SMEM(request.shape, jnp.int32),
            dma((7,)),
            dma((span_size,)),
            dma((span_size,)),
            dma((span_size,)),
            dma((span_size,)),
            dma((2, head_size, 2)),
            dma((2, head_size)),
            dma((2, head_size)),
            dma((2, head_size)),
            dma((chunks, head_size)),
            dma((chunks, head_size)),
            dma((chunks, head_size)),
            dma((chunks, head_size)),
            dma((chunks, head_size)),
            dma((chunks, head_size)),
        ],
        compiler_params=pltpu.CompilerParams(
            collective_id=0, has_side_effects=True, vmem_limit_bytes=VMEM
        ),
        cost_estimate=pl.CostEstimate(
            flops=6 * rows * model * head_size * group, bytes_accessed=16 << 20, transcendentals=0
        ),
    )(
        position,
        request,
        states.reshape(blocks, SPAN_LEN, model),
        encodings,
        query_weight,
        key_weight,
        value_weight,
        out_weight,
    )


def body(
    decoder_states, encodings, neighbor_table, query_weight, key_weight, value_weight, out_weight
):
    peer_count = lax.axis_size("span")
    shard_ids = neighbor_table[:, :, 0].reshape(-1)
    slot_ids = neighbor_table[:, :, 1].reshape(-1)
    entries = shard_ids.shape[0]
    per_peer = entries // peer_count
    numbering = jnp.arange(entries, dtype=jnp.int32)
    same_before = (shard_ids[:, None] == shard_ids[None, :]) & (
        numbering[None, :] < numbering[:, None]
    )
    ranking = jnp.sum(same_before.astype(jnp.int32), axis=1)
    position = shard_ids * per_peer + ranking
    placed = position[None, :] == numbering[:, None]
    request = jnp.sum(jnp.where(placed, slot_ids[None, :], 0), axis=1)
    request = request.reshape(peer_count, 1, per_peer)
    request = jnp.pad(request, ((0, 0), (0, 7), (0, 128 - per_peer)))
    out = fused(
        position,
        request,
        decoder_states,
        encodings,
        query_weight,
        key_weight,
        value_weight,
        out_weight,
    )
    return out.reshape(decoder_states.shape[0], -1)


def solution(mesh):
    return jax.shard_map(
        body,
        mesh=mesh,
        in_specs=(
            P("span", None),
            P("span", "head", None),
            P("span", None, None),
            P(None, "head"),
            P(None, "head"),
            P(None, "head"),
            P("head", None),
        ),
        out_specs=P("span", "head"),
        check_vma=False,
    )
```

```python
import functools

import jax
import jax.numpy as jnp
from jax import lax
from jax.experimental import pallas as pl
from jax.experimental.pallas import tpu as pltpu
from jax.sharding import PartitionSpec as P

HEAD_DIM = 64
SPAN_LEN = 64
SEQ_LEN = 2048
VMEM = 63 * 1024 * 1024
CHUNK_SPANS = 4
LINK = pl.DeviceIdType.MESH


def flip(index, bits, size):
    out = 0
    weight = 1
    while weight < size:
        out = out + weight * ((index // weight + bits // weight) % 2)
        weight *= 2
    return out


def kernel(
    span_size,
    head_size,
    rows_a,
    position_ref,
    order_ref,
    place_ref,
    request_ref,
    states_hbm,
    encodings_hbm,
    query_hbm,
    key_hbm,
    value_hbm,
    out_hbm,
    o_ref,
    enc,
    sent,
    arrived_a,
    arrived_b,
    arrived_c,
    weights,
    outs,
    states,
    queries,
    kv_a,
    kv_b,
    kv_c,
    own,
    right,
    left,
    lse,
    top,
    ctx,
    score,
    expo,
    final,
    asked,
    asked_s,
    local_sem,
    ask_send,
    ask_recv,
    enc_send,
    enc_recv,
    relay_send,
    relay_recv,
    line_send,
    line_recv,
    piece_send,
    piece_recv,
    pair_send,
    pair_recv,
    lse_send,
    lse_recv,
    right_send,
    right_recv,
    left_send,
    left_recv,
):
    me = lax.axis_index("span")
    plane = lax.axis_index("head")
    core = me % 2
    last = head_size - 1
    partner = me + 1 - 2 * core
    slots, tokens, model = encodings_hbm.shape
    per_peer = sent.shape[1]
    rows_b = per_peer - rows_a
    split = rows_b > 0
    middle = (plane > 0) & (plane < last)
    group = query_hbm.shape[1]

    own_copies = [
        pltpu.make_async_copy(key_hbm, weights.at[plane, :, 0:group], local_sem.at[0]),
        pltpu.make_async_copy(value_hbm, weights.at[plane, :, group : 2 * group], local_sem.at[1]),
        pltpu.make_async_copy(query_hbm, weights.at[plane, :, 2 * group : 3 * group], local_sem.at[2]),
        pltpu.make_async_copy(encodings_hbm, enc, local_sem.at[3]),
        pltpu.make_async_copy(states_hbm, states, local_sem.at[4]),
        pltpu.make_async_copy(out_hbm, outs.at[plane], local_sem.at[5]),
    ]
    for copy in own_copies:
        copy.start()
    asked[me] = request_ref[me]

    barrier = pltpu.get_barrier_semaphore()
    for k in range(1, span_size):
        pl.semaphore_signal(
            barrier, inc=1, device_id=(flip(me, k, span_size), plane), device_id_type=LINK
        )
    for k in range(1, head_size):
        pl.semaphore_signal(
            barrier, inc=1, device_id=(me, (plane + k) % head_size), device_id_type=LINK
        )
    pl.semaphore_wait(barrier, span_size + head_size - 2)

    def ask(k):
        peer = flip(me, k, span_size)
        return pltpu.make_async_remote_copy(
            src_ref=request_ref.at[peer],
            dst_ref=asked.at[me],
            send_sem=ask_send.at[k],
            recv_sem=ask_recv.at[k],
            device_id=(peer, plane),
            device_id_type=LINK,
        )

    def landed(k):
        peer = flip(me, k, span_size)
        return pltpu.make_async_remote_copy(
            src_ref=request_ref.at[peer],
            dst_ref=asked.at[peer],
            send_sem=ask_send.at[k],
            recv_sem=ask_recv.at[k],
            device_id=(peer, plane),
            device_id_type=LINK,
        )

    for k in range(1, span_size):
        ask(k).start()

    halves = ((weights, weights.shape[1] // 2, 0), (outs, outs.shape[1] // 2, 1))

    def line_copy(which, shard, to, direction):
        buf, half, slot = halves[which]
        rows = pl.ds(pl.multiple_of(core * half, half), half)
        return pltpu.make_async_remote_copy(
            src_ref=buf.at[shard, rows],
            dst_ref=buf.at[shard, rows],
            send_sem=line_send.at[slot, shard, direction],
            recv_sem=line_recv.at[slot, shard],
            device_id=(me, to),
            device_id_type=LINK,
        )

    bit_x, bit_y = (me // 2) % 2, (me // 4) % 2
    quarter = weights.shape[1] // 8

    def piece_copy(shard, piece, slot, to_span, to_plane):
        rows = pl.ds(pl.multiple_of(core * 4 * quarter + piece * quarter, quarter), quarter)
        return pltpu.make_async_remote_copy(
            src_ref=weights.at[shard, rows],
            dst_ref=weights.at[shard, rows],
            send_sem=piece_send.at[slot],
            recv_sem=piece_recv.at[slot],
            device_id=(to_span, to_plane),
            device_id_type=LINK,
        )

    def end_pieces(shard, to_plane):
        return (
            piece_copy(shard, 1 - bit_x, 0, me, to_plane),
            piece_copy(shard, 3 - bit_y, 1, me, to_plane),
        )

    def shared_pieces(shard):
        return (
            piece_copy(shard, 1 - bit_x, 2, flip(me, 2, span_size), plane),
            piece_copy(shard, 3 - bit_y, 3, flip(me, 4, span_size), plane),
        )

    def shared_landed(shard):
        return (
            piece_copy(shard, bit_x, 2, flip(me, 2, span_size), plane),
            piece_copy(shard, 2 + bit_y, 3, flip(me, 4, span_size), plane),
        )

    def far_shard(work):
        @pl.when((plane == 0) | (plane == last))
        def _():
            work(last - plane)

    def far_arrives(shard):
        for copy in end_pieces(shard, plane):
            copy.wait_recv()
        for copy in shared_pieces(shard):
            copy.start()

    def far_shared(shard):
        for copy in shared_landed(shard):
            copy.wait_recv()
        pair_copy(0, shard).start()

    def pair_copy(which, shard):
        buf, half, slot = halves[which]
        rows = pl.ds(pl.multiple_of(core * half, half), half)
        return pltpu.make_async_remote_copy(
            src_ref=buf.at[shard, rows],
            dst_ref=buf.at[shard, rows],
            send_sem=pair_send.at[slot, shard],
            recv_sem=pair_recv.at[slot, shard],
            device_id=(partner, plane),
            device_id_type=LINK,
        )

    def pair_landed(which, shard):
        buf, half, slot = halves[which]
        rows = pl.ds(pl.multiple_of((1 - core) * half, half), half)
        return pltpu.make_async_remote_copy(
            src_ref=buf.at[shard, rows],
            dst_ref=buf.at[shard, rows],
            send_sem=pair_send.at[slot, shard],
            recv_sem=pair_recv.at[slot, shard],
            device_id=(partner, plane),
            device_id_type=LINK,
        )

    def send_own(which):
        @pl.when(plane < last)
        def _():
            line_copy(which, plane, plane + 1, 0).start()

        @pl.when(plane > 0)
        def _():
            line_copy(which, plane, plane - 1, 1).start()

    def whole_hop(which, shard, to):
        if which == 1:
            return plane >= 0
        return (shard - to != last) & (to - shard != last)

    def pass_on(which, k):
        @pl.when(plane - k >= 0)
        def _():
            shard = plane - k
            line_copy(which, shard, plane, 0).wait_recv()

            @pl.when((plane < last) & whole_hop(which, shard, plane + 1))
            def _():
                line_copy(which, shard, plane + 1, 0).start()

            @pl.when((plane < last) & ~whole_hop(which, shard, plane + 1))
            def _():
                for copy in end_pieces(shard, plane + 1):
                    copy.start()

            pair_copy(which, shard).start()

        @pl.when(plane + k <= last)
        def _():
            shard = plane + k
            line_copy(which, shard, plane, 1).wait_recv()

            @pl.when((plane > 0) & whole_hop(which, shard, plane - 1))
            def _():
                line_copy(which, shard, plane - 1, 1).start()

            @pl.when((plane > 0) & ~whole_hop(which, shard, plane - 1))
            def _():
                for copy in end_pieces(shard, plane - 1):
                    copy.start()

            pair_copy(which, shard).start()

    for copy in own_copies[:3]:
        copy.wait()
    send_own(0)
    own_copies[5].wait()

    @pl.when(~middle)
    def _():
        send_own(1)


    for k in range(1, span_size):
        landed(k).wait_recv()
    to_scalar = pltpu.make_async_copy(asked, asked_s, local_sem.at[6])
    to_scalar.start()
    own_copies[3].wait()
    to_scalar.wait()

    def enc_copy(k, part):
        peer = flip(me, k, span_size)
        if part == 0:
            src, dst = sent.at[peer, pl.ds(0, rows_a)], arrived_a.at[me]
        else:
            src, dst = sent.at[peer, pl.ds(rows_a, rows_b)], arrived_b.at[me]
        return pltpu.make_async_remote_copy(
            src_ref=src,
            dst_ref=dst,
            send_sem=enc_send.at[part, k],
            recv_sem=enc_recv.at[part, k],
            device_id=(peer, plane),
            device_id_type=LINK,
        )

    def enc_landed(k, part):
        peer = flip(me, k, span_size)
        dst = (arrived_a, arrived_b)[part].at[peer]
        return pltpu.make_async_remote_copy(
            src_ref=dst,
            dst_ref=dst,
            send_sem=enc_send.at[part, k],
            recv_sem=enc_recv.at[part, k],
            device_id=(peer, plane),
            device_id_type=LINK,
        )

    mate = jnp.where(plane == 0, 1, last - 1)

    def relay_copy(k):
        peer = flip(me, k, span_size)
        return pltpu.make_async_remote_copy(
            src_ref=arrived_b.at[peer],
            dst_ref=arrived_c.at[peer],
            send_sem=relay_send.at[k],
            recv_sem=relay_recv.at[k],
            device_id=(me, mate),
            device_id_type=LINK,
        )

    def pick(buf, peer, offset, begin, count):
        for j in range(count):
            buf[peer, offset + j] = enc[asked_s[peer, 0, begin + j]]

    def pick_and_send(part, begin, count):
        def one(k, carry):
            pick(sent, flip(me, k, span_size), begin, begin, count)

            @pl.when(k > 1)
            def _():
                enc_copy(k - 1, part).start()

            return carry

        lax.fori_loop(1, span_size, one, 0)
        pick((arrived_a, arrived_b)[part], me, 0, begin, count)
        enc_copy(span_size - 1, part).start()

    if split:
        pick_and_send(1, rows_a, rows_b)
    pick_and_send(0, 0, rows_a)

    own_copies[4].wait()
    blocks, block_len, _ = states.shape
    blocks_seq = SEQ_LEN // block_len
    row = lax.broadcasted_iota(jnp.int32, (block_len, model), 0)

    def move_up(b, carry):
        inside = (b + 1) % blocks_seq != 0
        following = states[(b + 1) % blocks].astype(jnp.float32)
        following = jnp.where(inside, following, 0.0)
        tail = states[b].astype(jnp.float32)[block_len - 1 :]
        moved = jnp.where(row == 0, tail, pltpu.roll(following, 1, 0))
        states[b] = moved.astype(states.dtype)
        return carry

    lax.fori_loop(0, blocks, move_up, 0)

    def project_queries(shard):
        step = min(4, blocks)

        def one(b, carry):
            x = states[pl.ds(b * step, step)].reshape(step * block_len, model)
            y = jnp.dot(
                x, weights[shard, :, 2 * group : 3 * group], preferred_element_type=jnp.float32
            )
            queries[shard, pl.ds(b * step, step)] = y.astype(queries.dtype).reshape(
                step, block_len, group
            )
            return carry

        lax.fori_loop(0, blocks // step, one, 0)

    def project_keys(shard, src, dst, first, end):
        count = src.shape[1]

        def one(chip, carry):
            base = flip(me, 2 * chip, span_size) // 2 * 2
            x = src[pl.ds(base, 2)].reshape(2 * count * tokens, model)
            y = jnp.dot(x, weights[shard, :, 0 : 2 * group], preferred_element_type=jnp.float32)
            dst[shard, pl.ds(base * count, 2 * count)] = y.astype(dst.dtype).reshape(
                2 * count, tokens, 2 * group
            )
            return carry

        lax.fori_loop(first, end, one, 0)

    def shards_at(k, work):
        if k == 0:
            work(plane)
            return

        @pl.when(plane - k >= 0)
        def _():
            work(plane - k)

        @pl.when(plane + k <= last)
        def _():
            work(plane + k)

    chips = span_size // 2
    near, far = chips // 4, chips - chips // 4

    def keys_a(k, first, end):
        shards_at(k, lambda shard: project_keys(shard, arrived_a, kv_a, first, end))

    def keys_b(k, first, end):
        shards_at(k, lambda shard: project_keys(shard, arrived_b, kv_b, first, end))

    def keys_c(first, end):
        for shard in range(head_size):
            project_keys(shard, arrived_c, kv_c, first, end)

    def wait_enc(part, first, end):
        for k in range(max(2 * first, 1), 2 * end):
            enc_landed(k, part).wait_recv()

    def relay(first, end):
        if split:

            @pl.when(~middle)
            def _():
                wait_enc(1, first, end)
                for k in range(2 * first, 2 * end):
                    relay_copy(k).start()

    def relayed(first, end):
        for k in range(2 * first, 2 * end):
            relay_copy(k).wait_recv()

    def wait_pair(which, k):
        shards_at(k, lambda shard: pair_landed(which, shard).wait_recv())

    relay(0, near)
    project_queries(plane)
    wait_enc(0, 0, near)
    keys_a(0, 0, near)
    for k in range(1, last):
        pass_on(0, k)
        if k == last - 1:

            @pl.when(middle)
            def _():
                send_own(1)

        wait_pair(0, k)
        shards_at(k, project_queries)
        keys_a(k, 0, near)
        if k == 1:
            relay(near, far)
            relay(far, chips)
    far_shard(far_arrives)
    if split:
        @pl.when(middle)
        def _():
            wait_enc(1, 0, chips)
            for k in range(last):
                keys_b(k, 0, chips)

    wait_enc(0, near, far)
    for k in range(last):
        keys_a(k, near, far)
    @pl.when(middle)
    def _():
        for k in range(1, last):
            pass_on(1, k)

    wait_enc(0, far, chips)
    for k in range(last):
        keys_a(k, far, chips)
    far_shard(far_shared)
    wait_pair(0, last)
    shards_at(last, project_queries)
    keys_a(last, 0, chips)
    @pl.when(~middle)
    def _():
        for k in range(1, last):
            pass_on(1, k)

    pass_on(1, last)
    for k in range(1, head_size):
        wait_pair(1, k)
    if split:
        @pl.when(middle)
        def _():
            relayed(0, far)
            keys_c(0, far)


    chunks = blocks // CHUNK_SPANS
    chunk_spans = CHUNK_SPANS
    heads = head_size * group // HEAD_DIM
    neighbors = position_ref.shape[0] // blocks
    packed = group // HEAD_DIM
    lane = lax.broadcasted_iota(jnp.int32, (SPAN_LEN, 128), 1)

    def is_b(chunk):
        if not split:
            return chunk < 0
        return ((chunk >= 2) & (chunk % 2 == 0)) | (chunk == chunks - 1)

    def attend(chunk, sources):
        keys = neighbors * len(sources) * tokens
        wide = packed * keys
        cols = heads * keys
        pair = 128 // keys
        lane_head = lane // keys
        diagonal = (
            lax.broadcasted_iota(jnp.int32, (wide, group), 0) // keys
            == lax.broadcasted_iota(jnp.int32, (wide, group), 1) // HEAD_DIM
        )
        collect = (
            lax.broadcasted_iota(jnp.int32, (cols, 128), 0) // keys
            == lax.broadcasted_iota(jnp.int32, (cols, 128), 1)
        ).astype(jnp.bfloat16)

        def widened(c, g, base):
            part = jnp.concatenate(
                [
                    source[g, position_ref[(chunk * chunk_spans + c) * neighbors + n]][
                        :, base : base + group
                    ]
                    for n in range(neighbors)
                    for source in sources
                ],
                axis=0,
            )
            return jnp.where(diagonal, jnp.concatenate([part] * packed, axis=0), 0)

        for c in range(chunk_spans):
            rows = slice(c * SPAN_LEN, (c + 1) * SPAN_LEN)
            for g in range(head_size):
                score[rows, g * wide : (g + 1) * wide] = lax.dot_general(
                    queries[g, order_ref[chunk * chunk_spans + c]],
                    widened(c, g, 0),
                    (((1,), (1,)), ((), ())),
                    preferred_element_type=jnp.float32,
                ) * (HEAD_DIM ** (-0.5))
        tops = []
        for c in range(chunk_spans):
            rows = slice(c * SPAN_LEN, (c + 1) * SPAN_LEN)
            top_all = jnp.zeros((SPAN_LEN, 128), jnp.float32)
            for t in range(heads // pair):
                s = score[rows, t * 128 : (t + 1) * 128]
                if pair == 1:
                    peak = jnp.max(s, axis=1, keepdims=True)
                    top_all = jnp.where(lane == t, peak, top_all)
                else:
                    peak = None
                    for n in range(pair):
                        m = jnp.max(jnp.where(lane_head == n, s, -jnp.inf), axis=1, keepdims=True)
                        peak = m if peak is None else jnp.where(lane_head == n, m, peak)
                        top_all = jnp.where(lane == t * pair + n, m, top_all)
                expo[rows, t * 128 : (t + 1) * 128] = jnp.exp(s - peak).astype(jnp.bfloat16)
            tops.append(top_all)
        top_all = jnp.concatenate(tops, axis=0)
        total = jnp.dot(expo[:, :cols], collect, preferred_element_type=jnp.float32)
        top_rows = top_all.T[:heads]
        top[chunk % 2] = top_rows
        lse[plane, chunk] = top_rows + jnp.log(total.T[:heads])
        for c in range(chunk_spans):
            rows = slice(c * SPAN_LEN, (c + 1) * SPAN_LEN)
            for g in range(head_size):
                ctx[chunk % 2, rows, g * group : (g + 1) * group] = jnp.dot(
                    expo[rows, g * wide : (g + 1) * wide],
                    widened(c, g, group),
                    preferred_element_type=jnp.float32,
                ).astype(ctx.dtype)

    def lse_across(chunk):
        return pltpu.make_async_remote_copy(
            src_ref=lse.at[plane, chunk],
            dst_ref=lse.at[plane, chunk],
            send_sem=lse_send.at[chunk, 0],
            recv_sem=lse_recv.at[chunk, 0],
            device_id=(me, last - plane),
            device_id_type=LINK,
        )

    def lse_across_landed(chunk):
        return pltpu.make_async_remote_copy(
            src_ref=lse.at[last - plane, chunk],
            dst_ref=lse.at[last - plane, chunk],
            send_sem=lse_send.at[chunk, 0],
            recv_sem=lse_recv.at[chunk, 0],
            device_id=(me, last - plane),
            device_id_type=LINK,
        )

    def lse_copy(chunk, k):
        return pltpu.make_async_remote_copy(
            src_ref=lse.at[plane, chunk],
            dst_ref=lse.at[plane, chunk],
            send_sem=lse_send.at[chunk, k],
            recv_sem=lse_recv.at[chunk, k],
            device_id=(me, (plane + k) % head_size),
            device_id_type=LINK,
        )

    def lse_landed(chunk, k):
        origin = (plane + head_size - k) % head_size
        return pltpu.make_async_remote_copy(
            src_ref=lse.at[origin, chunk],
            dst_ref=lse.at[origin, chunk],
            send_sem=lse_send.at[chunk, k],
            recv_sem=lse_recv.at[chunk, k],
            device_id=(me, (plane + k) % head_size),
            device_id_type=LINK,
        )

    def project(chunk, first, end):
        every = lse[first:end, chunk]
        highest = jnp.max(every, axis=0)
        total = jnp.sum(jnp.exp(every - highest[None]), axis=0)
        scale = jnp.exp(top[chunk % 2] - highest) / total
        high = scale.astype(jnp.bfloat16)
        low = (scale - high.astype(jnp.float32)).astype(jnp.bfloat16)
        spread = (
            lax.broadcasted_iota(jnp.int32, (2 * heads, model), 0) % heads
            == lax.broadcasted_iota(jnp.int32, (2 * heads, model), 1) // HEAD_DIM
        ).astype(jnp.bfloat16)
        factor = lax.dot_general(
            jnp.concatenate([high, low], axis=0),
            spread,
            (((0,), (0,)), ((), ())),
            preferred_element_type=jnp.float32,
        )
        scaled = (ctx[chunk % 2].astype(jnp.float32) * factor).astype(jnp.bfloat16)
        w = outs[...].reshape(head_size * group, model)
        y = jnp.dot(scaled, w, preferred_element_type=jnp.float32)
        for q in range(head_size):
            own[chunk % head_size, q] = y[:, q * group : (q + 1) * group]

    def right_copy(chunk, q, to):
        return pltpu.make_async_remote_copy(
            src_ref=right.at[chunk, q - 1],
            dst_ref=right.at[chunk, q - 1],
            send_sem=right_send.at[chunk, q],
            recv_sem=right_recv.at[chunk, q],
            device_id=(me, to),
            device_id_type=LINK,
        )

    def left_copy(chunk, q, to):
        return pltpu.make_async_remote_copy(
            src_ref=left.at[chunk, q],
            dst_ref=left.at[chunk, q],
            send_sem=left_send.at[chunk, q],
            recv_sem=left_recv.at[chunk, q],
            device_id=(me, to),
            device_id_type=LINK,
        )

    def step(it, carry):
        @pl.when((it < chunks) & ~is_b(it))
        def _():
            attend(it, (kv_a,))
            for k in range(1, head_size):
                lse_copy(it, k).start()

        if split:

            @pl.when((it == 2) & middle)
            def _():
                relayed(far, chips)
                keys_c(far, chips)

            @pl.when((it < chunks) & is_b(it) & middle)
            def _():
                attend(it, (kv_b, kv_c))
                lse_across(it).start()

        before = it - 1

        @pl.when((before >= 0) & (before < chunks) & ~is_b(before))
        def _():
            for k in range(1, head_size):
                lse_landed(before, k).wait_recv()
            project(before, 0, head_size)

        if split:

            @pl.when((before >= 0) & (before < chunks) & is_b(before) & middle)
            def _():
                lse_across_landed(before).wait_recv()
                project(before, 1, last)

        to_right = it - 1 - plane
        right_b = is_b(to_right)
        right_on = (to_right >= 0) & (to_right < chunks) & (~right_b | middle)
        right_first = (plane == 0) | (right_b & (plane == 1))
        to_left = it - 1 - (last - plane)
        left_b = is_b(to_left)
        left_on = (to_left >= 0) & (to_left < chunks) & (~left_b | middle)
        left_first = (plane == last) | (left_b & (plane == last - 1))
        for q in range(head_size):
            if q > 0:

                @pl.when(right_on & (q > plane) & right_first)
                def _():
                    right[to_right, q - 1] = own[to_right % head_size, q].astype(right.dtype)

                @pl.when(right_on & (q > plane) & ~right_first)
                def _():
                    right_copy(to_right, q, plane).wait_recv()
                    right[to_right, q - 1] = (
                        own[to_right % head_size, q] + right[to_right, q - 1].astype(jnp.float32)
                    ).astype(right.dtype)

            if q < last:

                @pl.when(left_on & (q < plane) & left_first)
                def _():
                    left[to_left, q] = own[to_left % head_size, q].astype(left.dtype)

                @pl.when(left_on & (q < plane) & ~left_first)
                def _():
                    left_copy(to_left, q, plane).wait_recv()
                    left[to_left, q] = (
                        own[to_left % head_size, q] + left[to_left, q].astype(jnp.float32)
                    ).astype(left.dtype)

        for q in range(head_size):
            if q > 0:

                @pl.when(right_on & (q > plane))
                def _():
                    right_copy(to_right, q, plane + 1).start()

            if q < last:

                @pl.when(left_on & (q < plane))
                def _():
                    left_copy(to_left, q, plane - 1).start()

        done = it - 1 - jnp.maximum(plane, last - plane)
        done_b = is_b(done)
        done_on = (done >= 0) & (done < chunks)
        has_own = ~done_b | middle
        has_right = (plane > 1) | ((plane == 1) & ~done_b)
        has_left = (plane < last - 1) | ((plane == last - 1) & ~done_b)

        @pl.when(done_on)
        def _():
            @pl.when(has_left)
            def _():
                left_copy(done, plane, plane).wait_recv()

            @pl.when(has_right)
            def _():
                right_copy(done, plane, plane).wait_recv()

            def from_left_buffer():
                return left[done, jnp.minimum(plane, last - 1)].astype(jnp.float32)

            def from_right_buffer():
                return right[done, jnp.maximum(plane - 1, 0)].astype(jnp.float32)

            def mine():
                return own[done % head_size, plane]

            @pl.when(has_own & has_left & has_right)
            def _():
                put(done, mine() + from_left_buffer() + from_right_buffer())

            @pl.when(has_own & has_left & ~has_right)
            def _():
                put(done, mine() + from_left_buffer())

            @pl.when(has_own & ~has_left & has_right)
            def _():
                put(done, mine() + from_right_buffer())

            @pl.when(~has_own & has_left)
            def _():
                put(done, from_left_buffer())

            @pl.when(~has_own & has_right)
            def _():
                put(done, from_right_buffer())

        return carry

    def put(chunk, value):
        final[pl.ds(chunk * chunk_spans, chunk_spans)] = value.astype(final.dtype).reshape(
            chunk_spans, SPAN_LEN, group
        )

    lax.fori_loop(0, chunks + head_size, step, 0)

    out_row = lax.broadcasted_iota(jnp.int32, (SPAN_LEN, group), 0)

    def move_down(b, carry):
        previous = final[place_ref[(b + blocks - 1) % blocks]].astype(jnp.float32)
        before = jnp.where(b % blocks_seq != 0, previous, 0.0)
        here = final[place_ref[b]].astype(jnp.float32)
        moved = jnp.where(
            out_row == SPAN_LEN - 1, here[0:1], pltpu.roll(before, SPAN_LEN - 1, 0)
        )
        o_ref[b] = moved.astype(o_ref.dtype)
        return carry

    lax.fori_loop(0, blocks, move_down, 0)

    for k in range(1, span_size):
        ask(k).wait_send()
        enc_copy(k, 0).wait_send()
        if split:
            enc_copy(k, 1).wait_send()
    for which in range(2):

        @pl.when(plane < last)
        def _():
            line_copy(which, plane, plane + 1, 0).wait_send()

        @pl.when(plane > 0)
        def _():
            line_copy(which, plane, plane - 1, 1).wait_send()

        for k in range(1, head_size):

            @pl.when(plane - k >= 0)
            def _():
                shard = plane - k

                @pl.when((plane < last) & whole_hop(which, shard, plane + 1))
                def _():
                    line_copy(which, shard, plane + 1, 0).wait_send()

                @pl.when((plane < last) & ~whole_hop(which, shard, plane + 1))
                def _():
                    for copy in end_pieces(shard, plane + 1):
                        copy.wait_send()

                pair_copy(which, shard).wait_send()

            @pl.when(plane + k <= last)
            def _():
                shard = plane + k

                @pl.when((plane > 0) & whole_hop(which, shard, plane - 1))
                def _():
                    line_copy(which, shard, plane - 1, 1).wait_send()

                @pl.when((plane > 0) & ~whole_hop(which, shard, plane - 1))
                def _():
                    for copy in end_pieces(shard, plane - 1):
                        copy.wait_send()

                pair_copy(which, shard).wait_send()

    def far_sent(shard):
        for copy in shared_pieces(shard):
            copy.wait_send()

    far_shard(far_sent)
    if split:

        @pl.when(~middle)
        def _():
            for k in range(span_size):
                relay_copy(k).wait_send()


    def drain(chunk, carry):
        @pl.when(~is_b(chunk))
        def _():
            for k in range(1, head_size):
                lse_copy(chunk, k).wait_send()

        if split:

            @pl.when(is_b(chunk) & middle)
            def _():
                lse_across(chunk).wait_send()

        on = ~is_b(chunk) | middle
        for q in range(head_size):
            if q > 0:

                @pl.when(on & (q > plane))
                def _():
                    right_copy(chunk, q, plane + 1).wait_send()

            if q < last:

                @pl.when(on & (q < plane))
                def _():
                    left_copy(chunk, q, plane - 1).wait_send()

        return carry

    lax.fori_loop(0, chunks, drain, 0)


def fused(
    rows_a,
    position,
    order,
    place,
    request,
    states,
    encodings,
    query_weight,
    key_weight,
    value_weight,
    out_weight,
):
    span_size = lax.axis_size("span")
    head_size = lax.axis_size("head")
    slots, tokens, model = encodings.shape
    rows = states.shape[0]
    group = query_weight.shape[1]
    entries = position.shape[0]
    per_peer = entries // span_size
    rows_b = per_peer - rows_a
    held_b = max(rows_b, 1)
    blocks = rows // SPAN_LEN
    chunks = blocks // CHUNK_SPANS
    chunk_rows = CHUNK_SPANS * SPAN_LEN
    heads = head_size * group // HEAD_DIM
    score_cols = heads * (entries // blocks) * tokens * (2 if rows_b else 1)
    bf16, f32 = jnp.bfloat16, jnp.float32
    dma = pltpu.SemaphoreType.DMA
    vmem = pl.BlockSpec(memory_space=pltpu.VMEM)
    smem = pl.BlockSpec(memory_space=pltpu.SMEM)
    hbm = pl.BlockSpec(memory_space=pl.ANY)
    return pl.pallas_call(
        functools.partial(kernel, span_size, head_size, rows_a),
        out_shape=jax.ShapeDtypeStruct((blocks, SPAN_LEN, group), bf16),
        in_specs=[smem] * 3 + [vmem] + [hbm] * 6,
        out_specs=vmem,
        scratch_shapes=[
            pltpu.VMEM((slots, tokens, model), bf16),
            pltpu.VMEM((span_size, per_peer, tokens, model), bf16),
            pltpu.VMEM((span_size, rows_a, tokens, model), bf16),
            pltpu.VMEM((span_size if rows_b else 1, held_b, tokens, model), bf16),
            pltpu.VMEM((span_size if rows_b else 1, held_b, tokens, model), bf16),
            pltpu.VMEM((head_size, model, 3 * group), bf16),
            pltpu.VMEM((head_size, group, model), bf16),
            pltpu.VMEM((blocks, SPAN_LEN, model), bf16),
            pltpu.VMEM((head_size, blocks, SPAN_LEN, group), bf16),
            pltpu.VMEM((head_size, span_size * rows_a, tokens, 2 * group), bf16),
            pltpu.VMEM((head_size, max(span_size * rows_b, 1), tokens, 2 * group), bf16),
            pltpu.VMEM((head_size, max(span_size * rows_b, 1), tokens, 2 * group), bf16),
            pltpu.VMEM((head_size, head_size, chunk_rows, group), f32),
            pltpu.VMEM((chunks, head_size - 1, chunk_rows, group), bf16),
            pltpu.VMEM((chunks, head_size - 1, chunk_rows, group), bf16),
            pltpu.VMEM((head_size, chunks, heads, chunk_rows), f32),
            pltpu.VMEM((2, heads, chunk_rows), f32),
            pltpu.VMEM((2, chunk_rows, model), bf16),
            pltpu.VMEM((chunk_rows, score_cols), f32),
            pltpu.VMEM((chunk_rows, score_cols), bf16),
            pltpu.VMEM((blocks, SPAN_LEN, group), bf16),
            pltpu.VMEM(request.shape, jnp.int32),
            pltpu.SMEM(request.shape, jnp.int32),
            dma((7,)),
            dma((span_size,)),
            dma((span_size,)),
            dma((2, span_size)),
            dma((2, span_size)),
            dma((span_size,)),
            dma((span_size,)),
            dma((2, head_size, 2)),
            dma((2, head_size)),
            dma((4,)),
            dma((4,)),
            dma((2, head_size)),
            dma((2, head_size)),
            dma((chunks, head_size)),
            dma((chunks, head_size)),
            dma((chunks, head_size)),
            dma((chunks, head_size)),
            dma((chunks, head_size)),
            dma((chunks, head_size)),
        ],
        compiler_params=pltpu.CompilerParams(
            collective_id=0, has_side_effects=True, vmem_limit_bytes=VMEM
        ),
        cost_estimate=pl.CostEstimate(
            flops=6 * rows * model * head_size * group, bytes_accessed=16 << 20, transcendentals=0
        ),
    )(
        position,
        order,
        place,
        request,
        states.reshape(blocks, SPAN_LEN, model),
        encodings,
        query_weight,
        key_weight,
        value_weight,
        out_weight,
    )


def take(values, index):
    numbering = jnp.arange(values.shape[0], dtype=jnp.int32)
    return jnp.sum(jnp.where(index[:, None] == numbering[None, :], values[None, :], 0), axis=1)


def put_at(values, index):
    numbering = jnp.arange(values.shape[0], dtype=jnp.int32)
    return jnp.sum(jnp.where(index[None, :] == numbering[:, None], values[None, :], 0), axis=1)


def other_half(values):
    return values.reshape(-1, 2)[:, ::-1].reshape(-1)


def orbit_min(start, step, length):
    reach = 1
    while reach < length:
        start = jnp.minimum(start, take(start, step))
        reach *= 2
        if reach < length:
            step = take(step, step)
    return start


def earlier(same):
    numbering = jnp.arange(same.shape[0], dtype=jnp.int32)
    return jnp.sum((same & (numbering[None, :] < numbering[:, None])).astype(jnp.int32), axis=1)


def paired(same, rank):
    numbering = jnp.arange(rank.shape[0], dtype=jnp.int32)
    beside = rank + 1 - 2 * (rank % 2)
    return jnp.sum(jnp.where(same & (rank[None, :] == beside[:, None]), numbering[None, :], 0), axis=1)


def halve(shard_ids):
    entries = shard_ids.shape[0]
    numbering = jnp.arange(entries, dtype=jnp.int32)
    same = shard_ids[:, None] == shard_ids[None, :]
    beside = paired(same, earlier(same))
    low = orbit_min(numbering, beside + 1 - 2 * (beside % 2), entries // 2)
    enters = low > other_half(low)
    same = same & (enters[:, None] == enters[None, :])
    beside = paired(same, earlier(same))
    follow = beside + 1 - 2 * (beside % 2)
    low = orbit_min(numbering // 2, take(follow, follow), entries // 4)
    return (low > take(low, follow)).astype(jnp.int32)


def body(
    decoder_states, encodings, neighbor_table, query_weight, key_weight, value_weight, out_weight
):
    peer_count = lax.axis_size("span")
    head_size = lax.axis_size("head")
    spans, neighbors = neighbor_table.shape[:2]
    shard_ids = neighbor_table[:, :, 0].reshape(-1)
    slot_ids = neighbor_table[:, :, 1].reshape(-1)
    entries = shard_ids.shape[0]
    per_peer = entries // peer_count
    split = (
        neighbors == 2
        and per_peer % 4 == 0
        and head_size == 4
        and spans % (2 * CHUNK_SPANS) == 0
        and spans >= 4 * CHUNK_SPANS
    )
    rows_a = per_peer // 2 if split else per_peer
    same = shard_ids[:, None] == shard_ids[None, :]
    numbering = jnp.arange(spans, dtype=jnp.int32)
    if split:
        half = halve(shard_ids)
        ranking = earlier(same & (half[:, None] == half[None, :]))
        span_half = half.reshape(-1, 2)[:, 0]
        span_rank = earlier(span_half[:, None] == span_half[None, :])
        count = span_rank // CHUNK_SPANS
        chunks = spans // CHUNK_SPANS
        chunk = jnp.where(
            span_half == 0,
            jnp.maximum(2 * count - 1, 0),
            jnp.minimum(2 * count + 2, chunks - 1),
        )
        place = chunk * CHUNK_SPANS + span_rank % CHUNK_SPANS
        order = put_at(numbering, place)
        asked_at = shard_ids * per_peer + half * rows_a + ranking
        entry_place = (place[:, None] * 2 + jnp.arange(2, dtype=jnp.int32)[None, :]).reshape(-1)
        position = put_at(shard_ids * rows_a + ranking, entry_place)
    else:
        ranking = earlier(same)
        place = order = numbering
        asked_at = position = shard_ids * per_peer + ranking
    request = put_at(slot_ids, asked_at).reshape(peer_count, 1, per_peer)
    request = jnp.pad(request, ((0, 0), (0, 7), (0, 128 - per_peer)))
    out = fused(
        rows_a,
        position,
        order,
        place,
        request,
        decoder_states,
        encodings,
        query_weight,
        key_weight,
        value_weight,
        out_weight,
    )
    return out.reshape(decoder_states.shape[0], -1)


def solution(mesh):
    return jax.shard_map(
        body,
        mesh=mesh,
        in_specs=(
            P("span", None),
            P("span", "head", None),
            P("span", None, None),
            P(None, "head"),
            P(None, "head"),
            P(None, "head"),
            P("head", None),
        ),
        out_specs=P("span", "head"),
        check_vma=False,
    )
```

```python
import functools

import jax
import jax.numpy as jnp
from jax import lax
from jax.experimental import pallas as pl
from jax.experimental.pallas import tpu as pltpu
from jax.sharding import PartitionSpec as P

HEAD_DIM = 64
SPAN_LEN = 64
SEQ_LEN = 2048
VMEM = 63 * 1024 * 1024
CHUNK_SPANS = 2
AHEAD = 3
LINK = pl.DeviceIdType.MESH


def flip(index, bits, size):
    out = 0
    weight = 1
    while weight < size:
        out = out + weight * ((index // weight + bits // weight) % 2)
        weight *= 2
    return out


def kernel(
    span_size,
    head_size,
    rows_a,
    table_ref,
    states_hbm,
    encodings_hbm,
    query_hbm,
    key_hbm,
    value_hbm,
    out_hbm,
    o_ref,
    enc,
    sent,
    arrived_a,
    arrived_b,
    arrived_c,
    weights,
    outs,
    states,
    queries,
    kv_a,
    kv_b,
    kv_c,
    own_a,
    own_b,
    right,
    left,
    lse,
    top,
    score,
    expo,
    final,
    plan,
    asked,
    asked_s,
    local_sem,
    ask_send,
    ask_recv,
    enc_send,
    enc_recv,
    relay_send,
    relay_recv,
    line_send,
    line_recv,
    piece_send,
    piece_recv,
    pair_send,
    pair_recv,
    lse_send,
    lse_recv,
    right_send,
    right_recv,
    left_send,
    left_recv,
):
    me = lax.axis_index("span")
    plane = lax.axis_index("head")
    core = me % 2
    last = head_size - 1
    blocks = states.shape[0]
    partner = me + 1 - 2 * core
    slots, tokens, model = encodings_hbm.shape
    per_peer = sent.shape[1]
    rows_b = per_peer - rows_a
    split = rows_b > 0
    middle = (plane > 0) & (plane < last)
    group = query_hbm.shape[1]

    own_copies = [
        pltpu.make_async_copy(key_hbm, weights.at[plane, :, 0:group], local_sem.at[0]),
        pltpu.make_async_copy(value_hbm, weights.at[plane, :, group : 2 * group], local_sem.at[1]),
        pltpu.make_async_copy(query_hbm, weights.at[plane, :, 2 * group : 3 * group], local_sem.at[2]),
        pltpu.make_async_copy(encodings_hbm, enc, local_sem.at[3]),
        pltpu.make_async_copy(states_hbm, states, local_sem.at[4]),
        pltpu.make_async_copy(out_hbm, outs.at[plane], local_sem.at[5]),
    ]
    for copy in own_copies:
        copy.start()

    barrier = pltpu.get_barrier_semaphore()
    for k in range(1, span_size):
        pl.semaphore_signal(
            barrier, inc=1, device_id=(flip(me, k, span_size), plane), device_id_type=LINK
        )
    for k in range(1, head_size):
        pl.semaphore_signal(
            barrier, inc=1, device_id=(me, (plane + k) % head_size), device_id_type=LINK
        )
    pl.semaphore_wait(barrier, span_size + head_size - 2)

    def ask(k):
        peer = flip(me, k, span_size)
        return pltpu.make_async_remote_copy(
            src_ref=plan,
            dst_ref=asked.at[me],
            send_sem=ask_send.at[k],
            recv_sem=ask_recv.at[k],
            device_id=(peer, plane),
            device_id_type=LINK,
        )

    def landed(k):
        peer = flip(me, k, span_size)
        return pltpu.make_async_remote_copy(
            src_ref=plan,
            dst_ref=asked.at[peer],
            send_sem=ask_send.at[k],
            recv_sem=ask_recv.at[k],
            device_id=(peer, plane),
            device_id_type=LINK,
        )


    halves = ((weights, weights.shape[1] // 2, 0), (outs, outs.shape[1] // 2, 1))

    def line_copy(which, shard, to, direction):
        buf, half, slot = halves[which]
        rows = pl.ds(pl.multiple_of(core * half, half), half)
        return pltpu.make_async_remote_copy(
            src_ref=buf.at[shard, rows],
            dst_ref=buf.at[shard, rows],
            send_sem=line_send.at[slot, shard, direction],
            recv_sem=line_recv.at[slot, shard],
            device_id=(me, to),
            device_id_type=LINK,
        )

    bit_x, bit_y = (me // 2) % 2, (me // 4) % 2
    quarter = weights.shape[1] // 8

    def piece_copy(shard, piece, slot, to_span, to_plane):
        rows = pl.ds(pl.multiple_of(core * 4 * quarter + piece * quarter, quarter), quarter)
        return pltpu.make_async_remote_copy(
            src_ref=weights.at[shard, rows],
            dst_ref=weights.at[shard, rows],
            send_sem=piece_send.at[slot],
            recv_sem=piece_recv.at[slot],
            device_id=(to_span, to_plane),
            device_id_type=LINK,
        )

    def end_pieces(shard, to_plane):
        return (
            piece_copy(shard, 1 - bit_x, 0, me, to_plane),
            piece_copy(shard, 3 - bit_y, 1, me, to_plane),
        )

    def shared_pieces(shard):
        return (
            piece_copy(shard, 1 - bit_x, 2, flip(me, 2, span_size), plane),
            piece_copy(shard, 3 - bit_y, 3, flip(me, 4, span_size), plane),
        )

    def shared_landed(shard):
        return (
            piece_copy(shard, bit_x, 2, flip(me, 2, span_size), plane),
            piece_copy(shard, 2 + bit_y, 3, flip(me, 4, span_size), plane),
        )

    def far_shard(work):
        @pl.when((plane == 0) | (plane == last))
        def _():
            work(last - plane)

    def far_arrives(shard):
        for copy in end_pieces(shard, plane):
            copy.wait_recv()
        for copy in shared_pieces(shard):
            copy.start()

    def far_shared(shard):
        for copy in shared_landed(shard):
            copy.wait_recv()
        pair_copy(0, shard).start()

    def pair_copy(which, shard):
        buf, half, slot = halves[which]
        rows = pl.ds(pl.multiple_of(core * half, half), half)
        return pltpu.make_async_remote_copy(
            src_ref=buf.at[shard, rows],
            dst_ref=buf.at[shard, rows],
            send_sem=pair_send.at[slot, shard],
            recv_sem=pair_recv.at[slot, shard],
            device_id=(partner, plane),
            device_id_type=LINK,
        )

    def pair_landed(which, shard):
        buf, half, slot = halves[which]
        rows = pl.ds(pl.multiple_of((1 - core) * half, half), half)
        return pltpu.make_async_remote_copy(
            src_ref=buf.at[shard, rows],
            dst_ref=buf.at[shard, rows],
            send_sem=pair_send.at[slot, shard],
            recv_sem=pair_recv.at[slot, shard],
            device_id=(partner, plane),
            device_id_type=LINK,
        )

    def send_own(which):
        @pl.when(plane < last)
        def _():
            line_copy(which, plane, plane + 1, 0).start()

        @pl.when(plane > 0)
        def _():
            line_copy(which, plane, plane - 1, 1).start()

    def whole_hop(which, shard, to):
        if which == 1:
            return plane >= 0
        return (shard - to != last) & (to - shard != last)

    def pass_on(which, k):
        @pl.when(plane - k >= 0)
        def _():
            shard = plane - k
            line_copy(which, shard, plane, 0).wait_recv()

            @pl.when((plane < last) & whole_hop(which, shard, plane + 1))
            def _():
                line_copy(which, shard, plane + 1, 0).start()

            @pl.when((plane < last) & ~whole_hop(which, shard, plane + 1))
            def _():
                for copy in end_pieces(shard, plane + 1):
                    copy.start()

            pair_copy(which, shard).start()

        @pl.when(plane + k <= last)
        def _():
            shard = plane + k
            line_copy(which, shard, plane, 1).wait_recv()

            @pl.when((plane > 0) & whole_hop(which, shard, plane - 1))
            def _():
                line_copy(which, shard, plane - 1, 1).start()

            @pl.when((plane > 0) & ~whole_hop(which, shard, plane - 1))
            def _():
                for copy in end_pieces(shard, plane - 1):
                    copy.start()

            pair_copy(which, shard).start()

    for copy in own_copies[:3]:
        copy.wait()
    send_own(0)
    own_copies[5].wait()

    @pl.when(~middle)
    def _():
        send_own(1)


    entries = table_ref.shape[1]
    request, position, order, place = plan_rows(
        table_ref[0:1, :], table_ref[1:2, :], per_peer, rows_a, entries // blocks
    )
    plan[...] = jnp.zeros_like(plan)
    asked[me] = jnp.zeros(plan.shape, plan.dtype)
    plan[0:1, 0:entries] = request
    plan[1:2, 0:entries] = position
    plan[2:3, 0:entries] = order
    plan[3:4, 0:entries] = place
    asked[me, 0:1, 0:entries] = request
    asked[me, 1:2, 0:entries] = position
    asked[me, 2:3, 0:entries] = order
    asked[me, 3:4, 0:entries] = place
    for k in range(1, span_size):
        ask(k).start()

    for k in range(1, span_size):
        landed(k).wait_recv()
    to_scalar = pltpu.make_async_copy(asked, asked_s, local_sem.at[6])
    to_scalar.start()
    own_copies[3].wait()
    to_scalar.wait()

    def enc_copy(k, part):
        peer = flip(me, k, span_size)
        if part == 0:
            src, dst = sent.at[peer, pl.ds(0, rows_a)], arrived_a.at[me]
        else:
            src, dst = sent.at[peer, pl.ds(rows_a, rows_b)], arrived_b.at[me]
        return pltpu.make_async_remote_copy(
            src_ref=src,
            dst_ref=dst,
            send_sem=enc_send.at[part, k],
            recv_sem=enc_recv.at[part, k],
            device_id=(peer, plane),
            device_id_type=LINK,
        )

    def enc_landed(k, part):
        peer = flip(me, k, span_size)
        dst = (arrived_a, arrived_b)[part].at[peer]
        return pltpu.make_async_remote_copy(
            src_ref=dst,
            dst_ref=dst,
            send_sem=enc_send.at[part, k],
            recv_sem=enc_recv.at[part, k],
            device_id=(peer, plane),
            device_id_type=LINK,
        )

    mate = jnp.where(plane == 0, 1, last - 1)

    def relay_copy(k):
        peer = flip(me, k, span_size)
        return pltpu.make_async_remote_copy(
            src_ref=arrived_b.at[peer],
            dst_ref=arrived_c.at[peer],
            send_sem=relay_send.at[k],
            recv_sem=relay_recv.at[k],
            device_id=(me, mate),
            device_id_type=LINK,
        )

    def pick(buf, peer, offset, begin, count):
        for j in range(count):
            buf[peer, offset + j] = enc[asked_s[peer, 0, me * per_peer + begin + j]]

    def pick_and_send(part, begin, count):
        def one(k, carry):
            pick(sent, flip(me, k, span_size), begin, begin, count)

            @pl.when(k > 1)
            def _():
                enc_copy(k - 1, part).start()

            return carry

        lax.fori_loop(1, span_size, one, 0)
        pick((arrived_a, arrived_b)[part], me, 0, begin, count)
        enc_copy(span_size - 1, part).start()

    if split:
        pick_and_send(1, rows_a, rows_b)
    pick_and_send(0, 0, rows_a)

    own_copies[4].wait()
    block_len = states.shape[1]
    blocks_seq = SEQ_LEN // block_len
    row = lax.broadcasted_iota(jnp.int32, (block_len, model), 0)

    def move_up(b, carry):
        inside = (b + 1) % blocks_seq != 0
        following = states[(b + 1) % blocks].astype(jnp.float32)
        following = jnp.where(inside, following, 0.0)
        tail = states[b].astype(jnp.float32)[block_len - 1 :]
        moved = jnp.where(row == 0, tail, pltpu.roll(following, 1, 0))
        states[b] = moved.astype(states.dtype)
        return carry

    lax.fori_loop(0, blocks, move_up, 0)

    def project_queries(shard):
        step = min(16, blocks)

        def one(b, carry):
            x = states[pl.ds(b * step, step)].reshape(step * block_len, model)
            y = jnp.dot(
                x, weights[shard, :, 2 * group : 3 * group], preferred_element_type=jnp.float32
            )
            queries[shard, pl.ds(b * step, step)] = y.astype(queries.dtype).reshape(
                step, block_len, group
            )
            return carry

        lax.fori_loop(0, blocks // step, one, 0)

    def project_keys(shard, src, dst, first, end):
        count = src.shape[1]

        def one(chip, carry):
            base = flip(me, 2 * chip, span_size) // 2 * 2
            x = src[pl.ds(base, 2)].reshape(2 * count * tokens, model)
            y = jnp.dot(x, weights[shard, :, 0 : 2 * group], preferred_element_type=jnp.float32)
            dst[shard, pl.ds(base * count, 2 * count)] = y.astype(dst.dtype).reshape(
                2 * count, tokens, 2 * group
            )
            return carry

        lax.fori_loop(first, end, one, 0)

    def project_all_keys(shard, src, dst):
        count = src.shape[1]
        step = min(4, span_size)

        def one(i, carry):
            x = src[pl.ds(i * step, step)].reshape(step * count * tokens, model)
            y = jnp.dot(x, weights[shard, :, 0 : 2 * group], preferred_element_type=jnp.float32)
            dst[shard, pl.ds(i * step * count, step * count)] = y.astype(dst.dtype).reshape(
                step * count, tokens, 2 * group
            )
            return carry

        lax.fori_loop(0, span_size // step, one, 0)

    def shards_at(k, work):
        if k == 0:
            work(plane)
            return

        @pl.when(plane - k >= 0)
        def _():
            work(plane - k)

        @pl.when(plane + k <= last)
        def _():
            work(plane + k)

    chips = span_size // 2
    near, far = chips // 4, chips - chips // 4

    def keys_a(k, first, end):
        shards_at(k, lambda shard: project_keys(shard, arrived_a, kv_a, first, end))

    def keys_b(k):
        shards_at(k, lambda shard: project_all_keys(shard, arrived_b, kv_b))

    def keys_c(first, end):
        for shard in range(head_size):
            project_keys(shard, arrived_c, kv_c, first, end)

    def wait_enc(part, first, end):
        for k in range(max(2 * first, 1), 2 * end):
            enc_landed(k, part).wait_recv()

    def relay(first, end):
        if split:

            @pl.when(~middle)
            def _():
                wait_enc(1, first, end)
                for k in range(2 * first, 2 * end):
                    relay_copy(k).start()

    def relayed(first, end):
        for k in range(2 * first, 2 * end):
            relay_copy(k).wait_recv()

    def wait_pair(which, k):
        shards_at(k, lambda shard: pair_landed(which, shard).wait_recv())

    relay(0, near)
    project_queries(plane)
    wait_enc(0, 0, near)
    keys_a(0, 0, near)
    for k in range(1, last):
        pass_on(0, k)
        if k == last - 1:

            @pl.when(middle)
            def _():
                send_own(1)

        wait_pair(0, k)
        shards_at(k, project_queries)
        keys_a(k, 0, near)
        if k == 1:
            relay(near, far)
            relay(far, chips)
    far_shard(far_arrives)
    if split:
        @pl.when(middle)
        def _():
            wait_enc(1, 0, chips)
            for k in range(last):
                keys_b(k)

    wait_enc(0, near, far)
    for k in range(last):
        keys_a(k, near, far)
    @pl.when(middle)
    def _():
        for k in range(1, last):
            pass_on(1, k)

    wait_enc(0, far, chips)
    for k in range(last):
        keys_a(k, far, chips)
    far_shard(far_shared)
    wait_pair(0, last)
    shards_at(last, project_queries)
    shards_at(last, lambda shard: project_all_keys(shard, arrived_a, kv_a))

    chunks = blocks // CHUNK_SPANS
    chunk_spans = CHUNK_SPANS
    heads = head_size * group // HEAD_DIM
    neighbors = entries // blocks
    packed = group // HEAD_DIM
    lane = lax.broadcasted_iota(jnp.int32, (SPAN_LEN, 128), 1)

    chunks_b = chunks // 2 if split else 0
    chunks_a = chunks - chunks_b

    def attend(chunk, sources):
        keys = neighbors * len(sources) * tokens
        wide = packed * keys
        cols = heads * keys
        pair = 128 // keys
        lane_head = lane // keys
        diagonal = (
            lax.broadcasted_iota(jnp.int32, (wide, group), 0) // keys
            == lax.broadcasted_iota(jnp.int32, (wide, group), 1) // HEAD_DIM
        )
        collect = (
            lax.broadcasted_iota(jnp.int32, (cols, 128), 0) // keys
            == lax.broadcasted_iota(jnp.int32, (cols, 128), 1)
        ).astype(jnp.bfloat16)

        def widened(c, g, base):
            part = jnp.concatenate(
                [
                    source[g, asked_s[me, 1, (chunk * chunk_spans + c) * neighbors + n]][
                        :, base : base + group
                    ]
                    for n in range(neighbors)
                    for source in sources
                ],
                axis=0,
            )
            return jnp.where(diagonal, jnp.concatenate([part] * packed, axis=0), 0)

        for c in range(chunk_spans):
            rows = slice(c * SPAN_LEN, (c + 1) * SPAN_LEN)
            for g in range(head_size):
                score[rows, g * wide : (g + 1) * wide] = lax.dot_general(
                    queries[g, asked_s[me, 2, (chunk * chunk_spans + c) * neighbors]],
                    widened(c, g, 0),
                    (((1,), (1,)), ((), ())),
                    preferred_element_type=jnp.float32,
                ) * (HEAD_DIM ** (-0.5))
        tops = []
        for c in range(chunk_spans):
            rows = slice(c * SPAN_LEN, (c + 1) * SPAN_LEN)
            top_all = jnp.zeros((SPAN_LEN, 128), jnp.float32)
            for t in range(heads // pair):
                s = score[rows, t * 128 : (t + 1) * 128]
                if pair == 1:
                    peak = jnp.max(s, axis=1, keepdims=True)
                    top_all = jnp.where(lane == t, peak, top_all)
                else:
                    peak = None
                    for n in range(pair):
                        m = jnp.max(jnp.where(lane_head == n, s, -jnp.inf), axis=1, keepdims=True)
                        peak = m if peak is None else jnp.where(lane_head == n, m, peak)
                        top_all = jnp.where(lane == t * pair + n, m, top_all)
                expo[rows, t * 128 : (t + 1) * 128] = jnp.exp(s - peak).astype(jnp.bfloat16)
            tops.append(top_all)
        top_all = jnp.concatenate(tops, axis=0)
        total = jnp.dot(expo[:, :cols], collect, preferred_element_type=jnp.float32)
        top_rows = top_all.T[:heads]
        top[chunk] = top_rows
        lse[plane, chunk] = top_rows + jnp.log(total.T[:heads])
        for c in range(chunk_spans):
            rows = slice(c * SPAN_LEN, (c + 1) * SPAN_LEN)
            for g in range(head_size):
                states[chunk * chunk_spans + c, :, g * group : (g + 1) * group] = jnp.dot(
                    expo[rows, g * wide : (g + 1) * wide],
                    widened(c, g, group),
                    preferred_element_type=jnp.float32,
                ).astype(states.dtype)

    def lse_across(chunk):
        return pltpu.make_async_remote_copy(
            src_ref=lse.at[plane, chunk],
            dst_ref=lse.at[plane, chunk],
            send_sem=lse_send.at[chunk, 0],
            recv_sem=lse_recv.at[chunk, 0],
            device_id=(me, last - plane),
            device_id_type=LINK,
        )

    def lse_across_landed(chunk):
        return pltpu.make_async_remote_copy(
            src_ref=lse.at[last - plane, chunk],
            dst_ref=lse.at[last - plane, chunk],
            send_sem=lse_send.at[chunk, 0],
            recv_sem=lse_recv.at[chunk, 0],
            device_id=(me, last - plane),
            device_id_type=LINK,
        )

    def lse_copy(chunk, k):
        return pltpu.make_async_remote_copy(
            src_ref=lse.at[plane, chunk],
            dst_ref=lse.at[plane, chunk],
            send_sem=lse_send.at[chunk, k],
            recv_sem=lse_recv.at[chunk, k],
            device_id=(me, (plane + k) % head_size),
            device_id_type=LINK,
        )

    def lse_landed(chunk, k):
        origin = (plane + head_size - k) % head_size
        return pltpu.make_async_remote_copy(
            src_ref=lse.at[origin, chunk],
            dst_ref=lse.at[origin, chunk],
            send_sem=lse_send.at[chunk, k],
            recv_sem=lse_recv.at[chunk, k],
            device_id=(me, (plane + k) % head_size),
            device_id_type=LINK,
        )

    def project(chunk, first, end, own, slot):
        every = lse[first:end, chunk]
        highest = jnp.max(every, axis=0)
        total = jnp.sum(jnp.exp(every - highest[None]), axis=0)
        scale = jnp.exp(top[chunk] - highest) / total
        high = scale.astype(jnp.bfloat16)
        low = (scale - high.astype(jnp.float32)).astype(jnp.bfloat16)
        spread = (
            lax.broadcasted_iota(jnp.int32, (2 * heads, model), 0) % heads
            == lax.broadcasted_iota(jnp.int32, (2 * heads, model), 1) // HEAD_DIM
        ).astype(jnp.bfloat16)
        factor = lax.dot_general(
            jnp.concatenate([high, low], axis=0),
            spread,
            (((0,), (0,)), ((), ())),
            preferred_element_type=jnp.float32,
        )
        context = states[pl.ds(chunk * chunk_spans, chunk_spans)].reshape(factor.shape)
        scaled = (context.astype(jnp.float32) * factor).astype(jnp.bfloat16)
        w = outs[...].reshape(head_size * group, model)
        y = jnp.dot(scaled, w, preferred_element_type=jnp.float32)
        for q in range(head_size):
            own[slot, q] = y[:, q * group : (q + 1) * group]

    def right_copy(chunk, q, to):
        return pltpu.make_async_remote_copy(
            src_ref=right.at[chunk, q - 1],
            dst_ref=right.at[chunk, q - 1],
            send_sem=right_send.at[chunk, q],
            recv_sem=right_recv.at[chunk, q],
            device_id=(me, to),
            device_id_type=LINK,
        )

    def left_copy(chunk, q, to):
        return pltpu.make_async_remote_copy(
            src_ref=left.at[chunk, q],
            dst_ref=left.at[chunk, q],
            send_sem=left_send.at[chunk, q],
            recv_sem=left_recv.at[chunk, q],
            device_id=(me, to),
            device_id_type=LINK,
        )

    def combine(buf, copy, on, first, chunk, q, index, own, slot):
        @pl.when(on & first)
        def _():
            buf[chunk, index] = own[slot, q].astype(buf.dtype)

        @pl.when(on & ~first)
        def _():
            copy(chunk, q, plane).wait_recv()
            buf[chunk, index] = (own[slot, q] + buf[chunk, index].astype(jnp.float32)).astype(
                buf.dtype
            )

    def sums(base, to_right, right_on, right_first, to_left, left_on, left_first, own):
        depth = own.shape[0]
        for q in range(head_size):
            if q > 0:
                combine(
                    right,
                    right_copy,
                    right_on & (q > plane),
                    right_first,
                    base + to_right,
                    q,
                    q - 1,
                    own,
                    to_right % depth,
                )
            if q < last:
                combine(
                    left,
                    left_copy,
                    left_on & (q < plane),
                    left_first,
                    base + to_left,
                    q,
                    q,
                    own,
                    to_left % depth,
                )
        for q in range(head_size):
            if q > 0:

                @pl.when(right_on & (q > plane))
                def _():
                    right_copy(base + to_right, q, plane + 1).start()

            if q < last:

                @pl.when(left_on & (q < plane))
                def _():
                    left_copy(base + to_left, q, plane - 1).start()

    def finish(chunk, on, has_left, has_right, own, slot):
        @pl.when(on)
        def _():
            @pl.when(has_left)
            def _():
                left_copy(chunk, plane, plane).wait_recv()

            @pl.when(has_right)
            def _():
                right_copy(chunk, plane, plane).wait_recv()

            def left_sum():
                return left[chunk, jnp.minimum(plane, last - 1)].astype(jnp.float32)

            def right_sum():
                return right[chunk, jnp.maximum(plane - 1, 0)].astype(jnp.float32)

            mine = 0.0 if own is None else own[slot, plane]

            @pl.when(has_left & has_right)
            def _():
                put(chunk, mine + left_sum() + right_sum())

            @pl.when(has_left & ~has_right)
            def _():
                put(chunk, mine + left_sum())

            @pl.when(~has_left & has_right)
            def _():
                put(chunk, mine + right_sum())

    def attend_b(index):
        attend(chunks_a + index, (kv_b, kv_c))
        lse_across(chunks_a + index).start()

    def attend_a(chunk, carry):
        attend(chunk, (kv_a,))
        for k in range(1, head_size):
            lse_copy(chunk, k).start()
        return carry

    lax.fori_loop(0, min(AHEAD, chunks_a), attend_a, 0)
    @pl.when(~middle)
    def _():
        for k in range(1, last):
            pass_on(1, k)

    pass_on(1, last)
    for k in range(1, head_size):
        wait_pair(1, k)
    if split:

        @pl.when(middle)
        def _():
            relayed(0, far)
            keys_c(0, far)
            relayed(far, chips)
            keys_c(far, chips)
            attend_b(0)

    def step(it, carry):
        @pl.when(it < chunks_a)
        def _():
            for k in range(1, head_size):
                lse_landed(it, k).wait_recv()
            project(it, 0, head_size, own_a, it % head_size)

        to_right, to_left = it - plane, it - (last - plane)
        sums(
            0,
            to_right,
            (to_right >= 0) & (to_right < chunks_a),
            plane == 0,
            to_left,
            (to_left >= 0) & (to_left < chunks_a),
            plane == last,
            own_a,
        )
        if split:

            @pl.when((it < chunks_b) & middle)
            def _():
                lse_across_landed(chunks_a + it).wait_recv()
                project(chunks_a + it, 1, last, own_b, it % own_b.shape[0])

            right_b, left_b = it - (plane - 1), it - (last - 1 - plane)
            sums(
                chunks_a,
                right_b,
                (right_b >= 0) & (right_b < chunks_b) & middle,
                plane == 1,
                left_b,
                (left_b >= 0) & (left_b < chunks_b) & middle,
                plane == last - 1,
                own_b,
            )

            @pl.when((it + 1 < chunks_b) & middle)
            def _():
                attend_b(it + 1)

        @pl.when(it + AHEAD < chunks_a)
        def _():
            attend_a(it + AHEAD, 0)

        done = it - jnp.maximum(plane, last - plane)
        done_on = (done >= 0) & (done < chunks_a)
        finish(done, done_on, plane < last, plane > 0, own_a, done % head_size)
        if split:
            done = it - jnp.maximum(plane - 1, last - 1 - plane)
            done_on = (done >= 0) & (done < chunks_b)
            slot = done % own_b.shape[0]
            finish(
                chunks_a + done, done_on & middle, plane < last - 1, plane > 1, own_b, slot
            )
            finish(chunks_a + done, done_on & ~middle, plane == 0, plane == last, None, 0)
        return carry

    def put(chunk, value):
        final[pl.ds(chunk * chunk_spans, chunk_spans)] = value.astype(final.dtype).reshape(
            chunk_spans, SPAN_LEN, group
        )

    lax.fori_loop(0, chunks_a + last, step, 0)

    out_row = lax.broadcasted_iota(jnp.int32, (SPAN_LEN, group), 0)

    def move_down(b, carry):
        previous = final[asked_s[me, 3, (b + blocks - 1) % blocks * neighbors]].astype(jnp.float32)
        before = jnp.where(b % blocks_seq != 0, previous, 0.0)
        here = final[asked_s[me, 3, b * neighbors]].astype(jnp.float32)
        moved = jnp.where(
            out_row == SPAN_LEN - 1, here[0:1], pltpu.roll(before, SPAN_LEN - 1, 0)
        )
        o_ref[b] = moved.astype(o_ref.dtype)
        return carry

    lax.fori_loop(0, blocks, move_down, 0)

    for k in range(1, span_size):
        ask(k).wait_send()
        enc_copy(k, 0).wait_send()
        if split:
            enc_copy(k, 1).wait_send()
    for which in range(2):

        @pl.when(plane < last)
        def _():
            line_copy(which, plane, plane + 1, 0).wait_send()

        @pl.when(plane > 0)
        def _():
            line_copy(which, plane, plane - 1, 1).wait_send()

        for k in range(1, head_size):

            @pl.when(plane - k >= 0)
            def _():
                shard = plane - k

                @pl.when((plane < last) & whole_hop(which, shard, plane + 1))
                def _():
                    line_copy(which, shard, plane + 1, 0).wait_send()

                @pl.when((plane < last) & ~whole_hop(which, shard, plane + 1))
                def _():
                    for copy in end_pieces(shard, plane + 1):
                        copy.wait_send()

                pair_copy(which, shard).wait_send()

            @pl.when(plane + k <= last)
            def _():
                shard = plane + k

                @pl.when((plane > 0) & whole_hop(which, shard, plane - 1))
                def _():
                    line_copy(which, shard, plane - 1, 1).wait_send()

                @pl.when((plane > 0) & ~whole_hop(which, shard, plane - 1))
                def _():
                    for copy in end_pieces(shard, plane - 1):
                        copy.wait_send()

                pair_copy(which, shard).wait_send()

    def far_sent(shard):
        for copy in shared_pieces(shard):
            copy.wait_send()

    far_shard(far_sent)
    if split:

        @pl.when(~middle)
        def _():
            for k in range(span_size):
                relay_copy(k).wait_send()


    def drain(chunk, carry):
        @pl.when(chunk < chunks_a)
        def _():
            for k in range(1, head_size):
                lse_copy(chunk, k).wait_send()

        if split:

            @pl.when((chunk >= chunks_a) & middle)
            def _():
                lse_across(chunk).wait_send()

        on = (chunk < chunks_a) | middle
        for q in range(head_size):
            if q > 0:

                @pl.when(on & (q > plane))
                def _():
                    right_copy(chunk, q, plane + 1).wait_send()

            if q < last:

                @pl.when(on & (q < plane))
                def _():
                    left_copy(chunk, q, plane - 1).wait_send()

        return carry

    lax.fori_loop(0, chunks, drain, 0)


def fused(
    rows_a,
    table,
    states,
    encodings,
    query_weight,
    key_weight,
    value_weight,
    out_weight,
):
    span_size = lax.axis_size("span")
    head_size = lax.axis_size("head")
    slots, tokens, model = encodings.shape
    rows = states.shape[0]
    group = query_weight.shape[1]
    entries = table.shape[1]
    per_peer = entries // span_size
    rows_b = per_peer - rows_a
    held_b = max(rows_b, 1)
    blocks = rows // SPAN_LEN
    chunks = blocks // CHUNK_SPANS
    chunk_rows = CHUNK_SPANS * SPAN_LEN
    heads = head_size * group // HEAD_DIM
    score_cols = heads * (entries // blocks) * tokens * (2 if rows_b else 1)
    bf16, f32 = jnp.bfloat16, jnp.float32
    dma = pltpu.SemaphoreType.DMA
    vmem = pl.BlockSpec(memory_space=pltpu.VMEM)
    hbm = pl.BlockSpec(memory_space=pl.ANY)
    return pl.pallas_call(
        functools.partial(kernel, span_size, head_size, rows_a),
        out_shape=jax.ShapeDtypeStruct((blocks, SPAN_LEN, group), bf16),
        in_specs=[vmem] + [hbm] * 6,
        out_specs=vmem,
        scratch_shapes=[
            pltpu.VMEM((slots, tokens, model), bf16),
            pltpu.VMEM((span_size, per_peer, tokens, model), bf16),
            pltpu.VMEM((span_size, rows_a, tokens, model), bf16),
            pltpu.VMEM((span_size if rows_b else 1, held_b, tokens, model), bf16),
            pltpu.VMEM((span_size if rows_b else 1, held_b, tokens, model), bf16),
            pltpu.VMEM((head_size, model, 3 * group), bf16),
            pltpu.VMEM((head_size, group, model), bf16),
            pltpu.VMEM((blocks, SPAN_LEN, model), bf16),
            pltpu.VMEM((head_size, blocks, SPAN_LEN, group), bf16),
            pltpu.VMEM((head_size, span_size * rows_a, tokens, 2 * group), bf16),
            pltpu.VMEM((head_size, max(span_size * rows_b, 1), tokens, 2 * group), bf16),
            pltpu.VMEM((head_size, max(span_size * rows_b, 1), tokens, 2 * group), bf16),
            pltpu.VMEM((head_size, head_size, chunk_rows, group), f32),
            pltpu.VMEM((head_size - 2, head_size, chunk_rows, group), f32),
            pltpu.VMEM((chunks, head_size - 1, chunk_rows, group), bf16),
            pltpu.VMEM((chunks, head_size - 1, chunk_rows, group), bf16),
            pltpu.VMEM((head_size, chunks, heads, chunk_rows), f32),
            pltpu.VMEM((chunks, heads, chunk_rows), f32),
            pltpu.VMEM((chunk_rows, score_cols), f32),
            pltpu.VMEM((chunk_rows, score_cols), bf16),
            pltpu.VMEM((blocks, SPAN_LEN, group), bf16),
            pltpu.VMEM((8, 128), jnp.int32),
            pltpu.VMEM((span_size, 8, 128), jnp.int32),
            pltpu.SMEM((span_size, 8, 128), jnp.int32),
            dma((7,)),
            dma((span_size,)),
            dma((span_size,)),
            dma((2, span_size)),
            dma((2, span_size)),
            dma((span_size,)),
            dma((span_size,)),
            dma((2, head_size, 2)),
            dma((2, head_size)),
            dma((4,)),
            dma((4,)),
            dma((2, head_size)),
            dma((2, head_size)),
            dma((chunks, head_size)),
            dma((chunks, head_size)),
            dma((chunks, head_size)),
            dma((chunks, head_size)),
            dma((chunks, head_size)),
            dma((chunks, head_size)),
        ],
        compiler_params=pltpu.CompilerParams(
            collective_id=0, has_side_effects=True, vmem_limit_bytes=VMEM
        ),
        cost_estimate=pl.CostEstimate(
            flops=6 * rows * model * head_size * group, bytes_accessed=16 << 20, transcendentals=0
        ),
    )(
        table,
        states.reshape(blocks, SPAN_LEN, model),
        encodings,
        query_weight,
        key_weight,
        value_weight,
        out_weight,
    )


def plan_rows(shards, slots, per_peer, rows_a, neighbors):
    entries = shards.shape[1]
    shape = (entries, entries)
    down = lax.broadcasted_iota(jnp.int32, shape, 0)
    across = lax.broadcasted_iota(jnp.int32, shape, 1)
    numbering = lax.broadcasted_iota(jnp.int32, (entries, 1), 0)
    zero = jnp.zeros(shape, jnp.int32)

    def total(condition, values):
        return jnp.sum(jnp.where(condition, values, zero), axis=1, keepdims=True)

    def as_row(column):
        return jnp.sum(jnp.where(down == across, column, zero), axis=0, keepdims=True)

    def put_at(column, index):
        return jnp.sum(jnp.where(index == across, column, zero), axis=0, keepdims=True)

    def take(column, index):
        return total(index == across, as_row(column))

    def earlier(same):
        return total(same & (across < down), zero + 1)

    def beside(index):
        return index + 1 - 2 * (index % 2)

    def paired(same, rank):
        return total(same & (as_row(rank) == beside(rank)), across)

    def orbit_min(start, step, length):
        reach = 1
        while reach < length:
            start = jnp.minimum(start, take(start, step))
            reach *= 2
            if reach < length:
                step = take(step, step)
        return start

    shard = total(down == across, shards)
    slot = total(down == across, slots)
    same = shard == shards
    if rows_a < per_peer:
        low = orbit_min(numbering, beside(paired(same, earlier(same))), entries // 2)
        enters = (low > take(low, beside(numbering))).astype(jnp.int32)
        kin = same & (enters == as_row(enters))
        follow = beside(paired(kin, earlier(kin)))
        low = orbit_min(numbering // 2, take(follow, follow), entries // 4)
        half = (low > take(low, follow)).astype(jnp.int32)
    else:
        half = numbering * 0
    alike = half == as_row(half)
    rank = earlier(same & alike)
    place = half * (entries // neighbors // 2) + earlier(alike) // neighbors
    entry_place = place * neighbors + numbering % neighbors
    request = put_at(slot, shard * per_peer + half * rows_a + rank)
    position = put_at(shard * rows_a + rank, entry_place)
    order = put_at(numbering // neighbors, entry_place)
    return request, position, order, as_row(place)


def body(
    decoder_states, encodings, neighbor_table, query_weight, key_weight, value_weight, out_weight
):
    peer_count = lax.axis_size("span")
    spans, neighbors = neighbor_table.shape[:2]
    per_peer = spans * neighbors // peer_count
    split = (
        neighbors == 2
        and per_peer % 4 == 0
        and lax.axis_size("head") == 4
        and spans % (2 * CHUNK_SPANS) == 0
    )
    out = fused(
        per_peer // 2 if split else per_peer,
        neighbor_table.reshape(-1, 2).T,
        decoder_states,
        encodings,
        query_weight,
        key_weight,
        value_weight,
        out_weight,
    )
    return out.reshape(decoder_states.shape[0], -1)


def solution(mesh):
    return jax.shard_map(
        body,
        mesh=mesh,
        in_specs=(
            P("span", None),
            P("span", "head", None),
            P("span", None, None),
            P(None, "head"),
            P(None, "head"),
            P(None, "head"),
            P("head", None),
        ),
        out_specs=P("span", "head"),
        check_vma=False,
    )
```
